256 devices in a mesh: lon: 16 (over x, y), lat: 16 (over z, core).
Axes of the slice: x: 4, y: 4, z: 8, core: 2. Of those that a mesh axis runs over, the one named last changes fastest.
Arguments:
- meridional_speed: float32 [16, 1024, 4096], P(None, 'lat', 'lon'), may hold values from -6 to 6
- theta_field: float32 [16, 1024, 4096], P(None, 'lat', 'lon'), may hold values from -2 to 30
- tier_vertical_span: float32 [16], replicated, may hold values from 0.5 to 4
- grid_zonal_span: float32 [1024, 4096], P('lat', 'lon'), may hold values from 0.05 to 40
- grid_plan_extent: float32 [1024, 4096], P('lat', 'lon'), may hold values from 0.2 to 5
- ocean_energy_input: float32 [1024, 4096], P('lat', 'lon'), may hold values from -6 to 6
- ocean_tier_tally: int32 [1024, 4096], P('lat', 'lon'), may hold values from 0 to 16, as said below
- grid_region_label: int32 [1024, 4096], P('lat', 'lon'), may hold values from 0 to 3
- seam_matching_meridian: int32 [4096], P('lon'), may hold values from 0 to 4095, as said below
Outputs:
- class_transport: float32 [4, 1024, 128], P(None, 'lat')
- overturning: float32 [4, 1024, 16], P(None, 'lat')
- heat_transport: float32 [4, 1024], P(None, 'lat')
- implied_transport: float32 [4, 1024], P(None, 'lat')
The draws below stay inside these ranges and needn't reach their ends.
Inputs may be any that keep to these rules, and one draw needn't show every extreme that they name: `ocean_tier_tally`: one column, the same at every latitude, has at least one wet level, and every column of the northernmost row has at least one. seam_matching_meridian[i] = (c - i) mod 4096 for a c that each draw picks.
All inputs are finite; a program needn't handle non-finite values.
Results may differ from the reference program's by a relative error of at most 0.0003.
Values sent between devices are 32-bit elements; how exact they have to be, the bound alone decides.
No kernel may reach another device: no remote copies, remote signals or barrier semaphores. Data moves between devices by JAX's collectives and lax.ppermute only.
A program may use at most 64 MiB of HBM per device.

```python
import math
import jax
import jax.numpy as jnp
from jax import lax

LOCAL_PARALLELS = 64
VERTICAL_TIERS = 16
THERMAL_BINS = 128
OCEAN_REGIONS = 4
GRID_MERIDIANS = 4096
GRID_PARALLELS = 1024


def draw_grid_zonal_span(key, part):
    column = jnp.arange(GRID_MERIDIANS, dtype=jnp.float32)[None, :] / (GRID_MERIDIANS - 1.0)
    base_width = jnp.exp(jax.random.uniform(key, (GRID_PARALLELS, GRID_MERIDIANS), jnp.float32, jnp.log(0.3), jnp.log(3.0)))
    return (base_width * jnp.exp(jnp.log(3.0) * column)).astype(jnp.float32)


def draw_ocean_tier_tally(key, part):
    raw_depth = jax.random.randint(key, (GRID_PARALLELS, GRID_MERIDIANS), -(VERTICAL_TIERS // 3), VERTICAL_TIERS + 1, dtype=jnp.int32)
    col_depth = jnp.maximum(raw_depth, 0)
    wet_column = jax.random.randint(jax.random.fold_in(key, 11), (), 0, GRID_MERIDIANS, dtype=jnp.int32)
    column_ids = jnp.arange(GRID_MERIDIANS, dtype=jnp.int32)[None, :]
    row_ids = jnp.arange(GRID_PARALLELS, dtype=jnp.int32)[:, None]
    forced = (column_ids == wet_column) | (row_ids == GRID_PARALLELS - 1)
    return jnp.where(forced, jnp.maximum(col_depth, 1), col_depth).astype(jnp.int32)


def draw_seam_matching_meridian(key, part):
    centre = jax.random.randint(key, (), 0, GRID_MERIDIANS, dtype=jnp.int32)
    column_ids = jnp.arange(GRID_MERIDIANS, dtype=jnp.int32)
    return jnp.mod(centre - column_ids + GRID_MERIDIANS, GRID_MERIDIANS).astype(jnp.int32)


def place_ends(array, rng, least, largest):
    shape = array.shape
    spot = [jax.random.randint(jax.random.fold_in(rng, axis), (), 0, shape[axis]) for axis in range(len(shape))]
    array = array.at[tuple(spot)].set(least)
    longest = shape.index(max(shape))
    spot[longest] = (spot[longest] + 1) % shape[longest]
    return array.at[tuple(spot)].set(largest)


def level_of(own_key, dims, shards, low, largest):
    factor_of, own = 1.0, jax.random.fold_in(own_key, 6)
    for position, blocks in shards:
        draws = jnp.exp(jax.random.uniform(jax.random.fold_in(own, position), (blocks,), jnp.float32, low / len(shards), largest / len(shards)))
        factor_of = factor_of * jnp.repeat(draws, dims[position] // blocks).reshape([-1 if axis == position else 1 for axis in range(len(dims))])
    return factor_of


def gaussian(rng, shape, scale, bound, split=(), held_as=jnp.bfloat16):
    array = jax.random.normal(rng, shape, jnp.float32) * scale
    if len(split) > 0:
        array = level_of(rng, shape, split, -0.22, 0.18) * array
    return jnp.clip(array, min=-bound, max=bound).astype(held_as)


def setup_inputs(seed: int = 0) -> dict:
    splits = jax.random.split(jax.random.key(seed), 10)
    meridional_speed = gaussian(splits[0], (VERTICAL_TIERS, GRID_PARALLELS, GRID_MERIDIANS), 1.0, 6.0, ((1, 16), (2, 16)), jnp.float32)
    theta_field = jnp.clip(-2.0 + 32.0 * jax.random.uniform(splits[1], (VERTICAL_TIERS, GRID_PARALLELS, GRID_MERIDIANS), jnp.float32) ** level_of(splits[1], (VERTICAL_TIERS, GRID_PARALLELS, GRID_MERIDIANS), ((1, 16), (2, 16)), -0.2, 0.2), -2.0, 30.0)
    tier_vertical_span = jnp.clip(jnp.exp(jax.random.uniform(splits[2], (VERTICAL_TIERS,), jnp.float32, math.log(0.5), math.log(4.0))), 0.5, 4.0)
    grid_zonal_span = draw_grid_zonal_span(jax.random.fold_in(splits[9], 71), 0)
    grid_plan_extent = jnp.clip(jnp.exp(math.log(5.0) - 3.218876 * jax.random.uniform(splits[4], (GRID_PARALLELS, GRID_MERIDIANS), jnp.float32) ** level_of(splits[4], (GRID_PARALLELS, GRID_MERIDIANS), ((0, 16), (1, 16)), -0.2, 0.2)), 0.2, 5.0)
    ocean_energy_input = gaussian(splits[5], (GRID_PARALLELS, GRID_MERIDIANS), 1.0, 6.0, ((0, 16), (1, 16)), jnp.float32)
    ocean_tier_tally = draw_ocean_tier_tally(jax.random.fold_in(splits[9], 71), 0)
    grid_region_label = place_ends(jax.random.randint(splits[7], (GRID_PARALLELS, GRID_MERIDIANS), 0, OCEAN_REGIONS), jax.random.fold_in(splits[7], 1), 0, OCEAN_REGIONS - 1).astype(jnp.int32)
    seam_matching_meridian = draw_seam_matching_meridian(jax.random.fold_in(splits[9], 71), 0)
    return {"meridional_speed": meridional_speed, "theta_field": theta_field, "tier_vertical_span": tier_vertical_span, "grid_zonal_span": grid_zonal_span, "grid_plan_extent": grid_plan_extent, "ocean_energy_input": ocean_energy_input, "ocean_tier_tally": ocean_tier_tally, "grid_region_label": grid_region_label, "seam_matching_meridian": seam_matching_meridian}


THERMAL_FLOOR = -2.0
THERMAL_RANGE = 32.0

def vertical_aggregate_field(meridional_speed, theta_field, tier_vertical_span, grid_zonal_span, grid_plan_extent, ocean_energy_input, ocean_tier_tally, grid_region_label, subsequent_theta, subsequent_vertical_extent, theta_bucket_tally, region_tally):
    tier_ordinal, parallel_tally, meridian_tally = theta_field.shape
    poleward_theta = jnp.concatenate([theta_field[:, 1:, :], subsequent_theta[:, None, :]], axis=1)
    interface_theta = 0.5 * (theta_field + poleward_theta)
    north_depth = jnp.concatenate([ocean_tier_tally[1:, :], subsequent_vertical_extent[None, :]], axis=0)
    face_depth = jnp.minimum(ocean_tier_tally, north_depth)
    level_iota = lax.broadcasted_iota(jnp.int32, (tier_ordinal, 1, 1), 0)
    wet_mask = (level_iota < face_depth[None, :, :]).astype(jnp.float32)
    water_capacity = wet_mask * tier_vertical_span[:, None, None] * grid_zonal_span[None, :, :]
    mass_conveyance = water_capacity * meridional_speed
    bucket_spacing = THERMAL_RANGE / theta_bucket_tally
    placement_offset = jnp.clip((interface_theta - THERMAL_FLOOR) / bucket_spacing, 0.0, theta_bucket_tally - 1.0)
    lower_real_value = jnp.minimum(jnp.floor(placement_offset), theta_bucket_tally - 2.0)
    upper_interp_factor = placement_offset - lower_real_value
    parallel_ramp = lax.broadcasted_iota(jnp.int32, (1, parallel_tally, 1), 1)
    group_labels = (grid_region_label[None, :, :] * parallel_tally + parallel_ramp) * theta_bucket_tally + lower_real_value.astype(jnp.int32)
    group_labels = group_labels.reshape(-1)
    bucket_aggregate = jax.ops.segment_sum(jnp.concatenate([(mass_conveyance * (1.0 - upper_interp_factor)).reshape(-1), (mass_conveyance * upper_interp_factor).reshape(-1)]), jnp.concatenate([group_labels, group_labels + 1]), num_segments=region_tally * parallel_tally * theta_bucket_tally)
    bucket_aggregate = bucket_aggregate.reshape(region_tally, parallel_tally, theta_bucket_tally)
    basin_iota = lax.broadcasted_iota(jnp.int32, (region_tally, 1, 1), 0)
    bucket_membership = (grid_region_label[None, :, :] == basin_iota).astype(jnp.float32)
    level_sum = jnp.einsum('bji,kji->bjk', bucket_membership, mass_conveyance, precision=lax.Precision.HIGHEST)
    energy_aggregate = jnp.einsum('dwk,wk->dw', bucket_membership, lax.optimization_barrier(jnp.sum(mass_conveyance * interface_theta, axis=0)), precision=lax.Precision.HIGHEST)
    parallel_theta_field = lax.optimization_barrier(jnp.sum(water_capacity * interface_theta, axis=(0, 2)))
    row_wet = lax.optimization_barrier(jnp.sum(water_capacity, axis=(0, 2)))
    flux_rows = jnp.einsum('dwk,wk->dw', bucket_membership, ocean_energy_input * grid_plan_extent, precision=lax.Precision.HIGHEST)
    return (bucket_aggregate, level_sum, energy_aggregate, parallel_theta_field, row_wet, flux_rows)

def finish_rows(bucket_aggregate, level_sum, energy_aggregate, parallel_theta_field, row_wet, unit_scale):
    row_mean = parallel_theta_field / row_wet
    volume_total = lax.optimization_barrier(jnp.sum(level_sum, axis=2))
    heat_out = unit_scale / 16.0 * (energy_aggregate - volume_total * row_mean[None, :])
    stream = unit_scale * jnp.cumsum(level_sum, axis=2)
    return (unit_scale * bucket_aggregate, stream, heat_out)

def reference(meridional_speed, theta_field, tier_vertical_span, grid_zonal_span, grid_plan_extent, ocean_energy_input, ocean_tier_tally, grid_region_label, seam_matching_meridian):
    reflected_theta = jnp.take(theta_field[:, GRID_PARALLELS - 1, :], seam_matching_meridian, axis=1)
    mirror_depth = jnp.take(ocean_tier_tally[GRID_PARALLELS - 1, :], seam_matching_meridian, axis=0)
    unit_scale = math.sqrt(THERMAL_BINS / (GRID_MERIDIANS * VERTICAL_TIERS))

    def row_block(parallel_initial_offset):
        tile_theta_field = lax.dynamic_slice_in_dim(theta_field, parallel_initial_offset, LOCAL_PARALLELS, 1)
        tile_speed_field = lax.dynamic_slice_in_dim(meridional_speed, parallel_initial_offset, LOCAL_PARALLELS, 1)
        tile_vertical_extent = lax.dynamic_slice_in_dim(ocean_tier_tally, parallel_initial_offset, LOCAL_PARALLELS, 0)
        tile_zonal_span = lax.dynamic_slice_in_dim(grid_zonal_span, parallel_initial_offset, LOCAL_PARALLELS, 0)
        tile_plan_extent = lax.dynamic_slice_in_dim(grid_plan_extent, parallel_initial_offset, LOCAL_PARALLELS, 0)
        tile_energy_input = lax.dynamic_slice_in_dim(ocean_energy_input, parallel_initial_offset, LOCAL_PARALLELS, 0)
        tile_region_label = lax.dynamic_slice_in_dim(grid_region_label, parallel_initial_offset, LOCAL_PARALLELS, 0)
        subsequent_offset = jnp.minimum(parallel_initial_offset + LOCAL_PARALLELS, GRID_PARALLELS - 1).astype(jnp.int32)
        final_flag = parallel_initial_offset + LOCAL_PARALLELS >= GRID_PARALLELS
        next_theta_value = lax.dynamic_slice_in_dim(theta_field, subsequent_offset, 1, 1)[:, 0, :]
        later_vertical_extent = lax.dynamic_slice_in_dim(ocean_tier_tally, subsequent_offset, 1, 0)[0]
        next_theta_value = jnp.where(final_flag, reflected_theta, next_theta_value)
        later_vertical_extent = jnp.where(final_flag, mirror_depth, later_vertical_extent)
        return vertical_aggregate_field(tile_speed_field, tile_theta_field, tier_vertical_span, tile_zonal_span, tile_plan_extent, tile_energy_input, tile_vertical_extent, tile_region_label, next_theta_value, later_vertical_extent, THERMAL_BINS, OCEAN_REGIONS)
    starts = jnp.arange(GRID_PARALLELS // LOCAL_PARALLELS, dtype=jnp.int32) * LOCAL_PARALLELS
    bucket_aggregate, level_sum, energy_aggregate, parallel_theta_field, row_wet, flux_rows = lax.map(row_block, starts)
    bucket_aggregate = jnp.transpose(bucket_aggregate, (1, 0, 2, 3)).reshape(OCEAN_REGIONS, GRID_PARALLELS, THERMAL_BINS)
    level_sum = jnp.transpose(level_sum, (1, 0, 2, 3)).reshape(OCEAN_REGIONS, GRID_PARALLELS, VERTICAL_TIERS)
    energy_aggregate = jnp.transpose(energy_aggregate, (1, 0, 2)).reshape(OCEAN_REGIONS, GRID_PARALLELS)
    flux_rows = jnp.transpose(flux_rows, (1, 0, 2)).reshape(OCEAN_REGIONS, GRID_PARALLELS)
    parallel_theta_field = parallel_theta_field.reshape(GRID_PARALLELS)
    row_wet = row_wet.reshape(GRID_PARALLELS)
    class_out, stream, heat_out = finish_rows(bucket_aggregate, level_sum, energy_aggregate, parallel_theta_field, row_wet, unit_scale)
    implied = 2.0 / math.sqrt(GRID_MERIDIANS * GRID_PARALLELS) * jnp.cumsum(flux_rows, axis=1)
    return (class_out, stream, heat_out, implied)
```

```python
import functools
import math

import jax
import jax.numpy as jnp
from jax import lax
from jax.experimental import pallas as pl
from jax.experimental.pallas import tpu as pltpu
from jax.sharding import PartitionSpec as P

THERMAL_BINS = 128
OCEAN_REGIONS = 4
THERMAL_FLOOR = -2.0
THERMAL_RANGE = 32.0

ROWS = 8
LOW = 8
HIGH = THERMAL_BINS // LOW
GROUPS = OCEAN_REGIONS * HIGH
LANES = 128
EDGE = 24
PARCEL = 24
HEAT, FLUX, SOUTH, MEAN, WET = 64, 68, 72, 76, 77


def split_in_two(x):
    high = x.astype(jnp.bfloat16).astype(jnp.float32)
    return high, x - high


def bin_rows(
    theta, speed, tier, zonal, plan, energy, depth, label, next_row, next_depth, parts, parcel
):
    levels = theta.shape[0]
    width = theta.shape[2]
    row_id = lax.broadcasted_iota(jnp.int32, (ROWS, width), 0)
    last_row = row_id == ROWS - 1

    def northern(own, beyond):
        return jnp.where(last_row, beyond, pltpu.roll(own, ROWS - 1, 0))

    own_depth = depth[...].astype(jnp.float32)
    face_depth = jnp.minimum(own_depth, northern(own_depth, next_depth()))
    basin = label[...]
    basin_base = basin.astype(jnp.float32) * float(HIGH)
    in_basin = [basin == b for b in range(OCEAN_REGIONS)]
    span = zonal[...]
    lane = lax.broadcasted_iota(jnp.int32, (ROWS, LANES), 1)
    terms = jnp.zeros((ROWS, LANES), jnp.float32)

    def over_longitude(x):
        return jnp.sum(x, axis=1, keepdims=True)

    running = [jnp.zeros((ROWS, 1), jnp.float32) for _ in range(OCEAN_REGIONS)]
    mean_sum = jnp.zeros((ROWS, width), jnp.float32)
    wet_sum = jnp.zeros((ROWS, width), jnp.float32)
    heat_sum = jnp.zeros((ROWS, width), jnp.float32)
    per_bin = THERMAL_BINS / THERMAL_RANGE
    for k in range(levels):
        own = theta[k]
        face = 0.5 * (own + northern(own, next_row(k)))
        volume = jnp.where(face_depth > float(k), tier[k] * span, 0.0)
        transport = volume * speed[k]
        position = jnp.clip((face - THERMAL_FLOOR) * per_bin, 0.0, THERMAL_BINS - 1.0)
        low_bin = jnp.minimum(jnp.floor(position), THERMAL_BINS - 2.0)
        high_weight = position - low_bin
        digit = jnp.floor(low_bin * (1.0 / LOW))
        weighted = transport * high_weight
        parts[0, k] = basin_base + digit
        parts[1, k] = low_bin - LOW * digit
        parts[2, k], parts[3, k] = split_in_two(transport)
        parts[4, k], parts[5, k] = split_in_two(weighted)
        mean_sum += volume * face
        wet_sum += volume
        heat_sum += transport * face
        for b in range(OCEAN_REGIONS):
            running[b] += over_longitude(jnp.where(in_basin[b], transport, 0.0))
            terms = jnp.where(lane == b * levels + k, running[b], terms)
    flux = energy[...] * plan[...]
    for b in range(OCEAN_REGIONS):
        terms = jnp.where(
            lane == HEAT + b, over_longitude(jnp.where(in_basin[b], heat_sum, 0.0)), terms
        )
        terms = jnp.where(
            lane == FLUX + b, over_longitude(jnp.where(in_basin[b], flux, 0.0)), terms
        )
    terms = jnp.where(lane == MEAN, over_longitude(mean_sum), terms)
    terms = jnp.where(lane == WET, over_longitude(wet_sum), terms)

    packed_id = lax.broadcasted_iota(jnp.int32, (16, width), 0)
    group_ids = [
        (packed_id + 16 * t).astype(jnp.float32).astype(jnp.bfloat16) for t in range(GROUPS // 16)
    ]
    low_ids = (packed_id & (LOW - 1)).astype(jnp.float32).astype(jnp.bfloat16)
    one = jnp.ones((16, width), jnp.bfloat16)
    none = jnp.zeros((16, width), jnp.bfloat16)

    def spread(q, k, r, count):
        return jnp.broadcast_to(parts[q, k, r : r + 1, :], (count, width))

    sums = []
    for r in range(ROWS):
        values, groups = [], []
        for k in range(levels):
            group = spread(0, k, r, 16).astype(jnp.bfloat16)
            groups.append(
                jnp.concatenate([jnp.where(group == g, one, none) for g in group_ids], axis=0)
            )
            at_low = spread(1, k, r, 16).astype(jnp.bfloat16) == low_ids
            pair = [
                jnp.concatenate([spread(q, k, r, 8), spread(q + 1, k, r, 8)], axis=0).astype(
                    jnp.bfloat16
                )
                for q in (2, 4)
            ]
            values.append(
                jnp.concatenate([jnp.where(at_low, v, none) for v in pair], axis=0)
            )
        sums.append(
            lax.dot_general(
                jnp.concatenate(values, axis=1),
                jnp.concatenate(groups, axis=1),
                (((1,), (1,)), ((), ())),
                preferred_element_type=jnp.float32,
            )
        )

    low_id = lax.broadcasted_iota(jnp.int32, (LOW, LANES), 0)
    classes = []
    for r in range(0, ROWS, 2):
        both = jnp.concatenate([sums[r], sums[r + 1]], axis=1)
        plain = both[0:8] + both[8:16]
        upper = both[16:24] + both[24:32]
        moved = pltpu.roll(upper, 1, 0)
        moved = jnp.where(low_id == 0, pltpu.roll(moved, 1, 1), moved)
        classes.append(plain - upper + moved)

    place_id = lax.broadcasted_iota(jnp.int32, (16, LANES), 0)
    lane16 = lax.broadcasted_iota(jnp.int32, (16, LANES), 1)
    of_place = (place_id & 1) * OCEAN_REGIONS + (place_id >> 2) == (lane16 >> 4)
    first = of_place & ((place_id & 2) == 0)
    second = of_place & ((place_id & 2) != 0)
    zero = jnp.zeros((16, LANES), jnp.float32)
    from_id = lax.broadcasted_iota(jnp.int32, (LANES, LANES), 0)
    to_id = lax.broadcasted_iota(jnp.int32, (LANES, LANES), 1)
    target = (from_id & (HIGH - 1)) * LOW
    placing = jnp.concatenate(
        [jnp.where(to_id == target + low, 1.0, 0.0) for low in range(LOW)], axis=0
    ).astype(jnp.bfloat16)
    rows = []
    for d in range(2):
        rows.append(
            jnp.concatenate(
                [
                    jnp.where(
                        first,
                        jnp.broadcast_to(classes[2 * d][low : low + 1], (16, LANES)),
                        jnp.where(
                            second,
                            jnp.broadcast_to(classes[2 * d + 1][low : low + 1], (16, LANES)),
                            zero,
                        ),
                    )
                    for low in range(LOW)
                ],
                axis=1,
            )
        )
    wide = jnp.concatenate(rows, axis=0)
    wide_high, wide_low = split_in_two(wide)
    placed = jnp.dot(
        jnp.concatenate([wide_high, wide_low], axis=0).astype(jnp.bfloat16),
        placing,
        preferred_element_type=jnp.float32,
    )
    placed = placed[0:32] + placed[32:64]
    for d in range(2):
        parcel[d, 0:16, :] = placed[16 * d : 16 * d + 16]
    return terms


def store_terms(parcel, terms):
    parcel[0, 16:24, :] = terms
    parcel[1, 16:24, :] = pltpu.roll(terms, 4, 0)


def early_kernel(
    theta, beyond, speed, tier, zonal, plan, energy, depth, depth_beyond, label, parcel, parts
):
    terms = bin_rows(
        theta,
        speed,
        tier,
        zonal,
        plan,
        energy,
        depth,
        label,
        lambda k: jnp.broadcast_to(beyond[k, 0:1, :], theta.shape[1:]),
        lambda: jnp.broadcast_to(depth_beyond[0:1, :], theta.shape[1:]).astype(jnp.float32),
        parts,
        parcel,
    )
    store_terms(parcel, terms)


def late_kernel(
    where_to,
    theta,
    speed,
    tier,
    zonal,
    plan,
    energy,
    depth,
    label,
    halo,
    fold_a,
    fold_b,
    south,
    so_far,
    parcel,
    parts,
    edge,
):
    del so_far
    shape = theta.shape[1:]
    width = shape[1]
    columns = jnp.concatenate([fold_a[0], fold_b[0]], axis=1)
    high, rest = split_in_two(columns)
    middle, lowest = split_in_two(rest)
    source = lax.broadcasted_iota(jnp.int32, (2 * width, width), 0)
    target = lax.broadcasted_iota(jnp.int32, (2 * width, width), 1)
    mirror = jnp.where(source + target == where_to[2] + (width - 1), 1.0, 0.0).astype(jnp.bfloat16)
    pieces = jnp.dot(
        jnp.concatenate([high, middle, lowest], axis=0).astype(jnp.bfloat16),
        mirror,
        preferred_element_type=jnp.float32,
    )
    folded = pieces[0:EDGE] + pieces[EDGE : 2 * EDGE] + pieces[2 * EDGE : 3 * EDGE]
    edge[...] = jnp.where(where_to[3] == 1, folded, halo[...])
    levels = theta.shape[0]
    terms = bin_rows(
        theta,
        speed,
        tier,
        zonal,
        plan,
        energy,
        depth,
        label,
        lambda k: jnp.broadcast_to(edge[k : k + 1, :], shape),
        lambda: jnp.broadcast_to(edge[levels : levels + 1, :], shape),
        parts,
        parcel,
    )
    further = lax.broadcasted_iota(jnp.int32, south.shape, 0) < where_to[4]
    offset = jnp.sum(jnp.where(further, south[...], 0.0), axis=0, keepdims=True)
    last = lax.broadcasted_iota(jnp.int32, terms.shape, 0) == ROWS - 1
    terms = terms + jnp.where(last, jnp.broadcast_to(offset, terms.shape), 0.0)
    store_terms(parcel, terms)


def finish_kernel(unit_scale, implied_scale, parcels, class_out, stream, heat, implied):
    devices = parcels.shape[0]
    rows = 4 * devices
    levels = stream.shape[2]
    for b in range(OCEAN_REGIONS):
        for d in range(devices):
            class_out[b, 4 * d : 4 * d + 4, :] = unit_scale * parcels[d, 4 * b : 4 * b + 4, :]
    terms = jnp.concatenate([parcels[d, 16:20, :] for d in range(devices)], axis=0)
    for b in range(OCEAN_REGIONS):
        stream[b] = unit_scale * terms[:, b * levels : (b + 1) * levels]
    turned = jnp.transpose(
        jnp.concatenate([terms, jnp.zeros((LANES - rows, LANES), jnp.float32)], axis=0)
    )
    row_mean = turned[MEAN : MEAN + 1] / jnp.where(
        lax.broadcasted_iota(jnp.int32, (1, LANES), 1) < rows, turned[WET : WET + 1], 1.0
    )
    lane = lax.broadcasted_iota(jnp.int32, (1, LANES), 1)
    for b in range(OCEAN_REGIONS):
        total = turned[(b + 1) * levels - 1 : (b + 1) * levels]
        out = unit_scale / 16.0 * (turned[HEAT + b : HEAT + b + 1] - total * row_mean)
        heat[b : b + 1, :] = out[:, :rows]
        flux = turned[FLUX + b : FLUX + b + 1]
        offset = jnp.sum(turned[SOUTH + b : SOUTH + b + 1], axis=1, keepdims=True)
        shift = 1
        while shift < rows:
            flux = flux + jnp.where(lane >= shift, pltpu.roll(flux, shift, 1), 0.0)
            shift *= 2
        implied[b : b + 1, :] = (implied_scale * (flux + offset))[:, :rows]


def exchanged(pieces, axis):
    return lax.all_to_all(pieces, axis, split_axis=0, concat_axis=0, tiled=True)


def copies(array, axis):
    return jnp.broadcast_to(array, (lax.axis_size(axis), *array.shape))


def body(
    meridional_speed,
    theta_field,
    tier_vertical_span,
    grid_zonal_span,
    grid_plan_extent,
    ocean_energy_input,
    ocean_tier_tally,
    grid_region_label,
    seam_matching_meridian,
):
    levels, parallels, width = theta_field.shape
    lon_size = lax.axis_size("lon")
    lat_size = lax.axis_size("lat")
    lat_index = lax.axis_index("lat")
    width_total = width * lon_size
    unit_scale = math.sqrt(THERMAL_BINS / (width_total * levels))
    implied_scale = 2.0 / math.sqrt(width_total * parallels * lat_size)
    blocks = parallels // ROWS

    def edge_of(row):
        depth = ocean_tier_tally[row][None].astype(jnp.float32)
        return jnp.concatenate(
            [theta_field[:, row, :], depth, jnp.zeros((EDGE - levels - 1, width), jnp.float32)]
        )

    halo = lax.ppermute(edge_of(0), "lat", [(i + 1, i) for i in range(lat_size - 1)])
    fold = exchanged(copies(edge_of(parallels - 1), "lon"), "lon")
    flux = ocean_energy_input * grid_plan_extent
    flux_totals = jnp.stack(
        [jnp.sum(jnp.where(grid_region_label == b, flux, 0.0)) for b in range(OCEAN_REGIONS)]
    )
    flux_lanes = jnp.pad(flux_totals, (SOUTH, LANES - SOUTH - OCEAN_REGIONS))
    south = exchanged(copies(flux_lanes, "lat"), "lat")

    start = (seam_matching_meridian[0] + (width_total - (width - 1))) % width_total
    first = start // width
    where_to = jnp.stack(
        [
            first,
            (first + 1) % lon_size,
            start % width,
            (lat_index == lat_size - 1).astype(jnp.int32),
            lat_index.astype(jnp.int32),
        ]
    )

    def field(index):
        return pl.BlockSpec((levels, ROWS, width), lambda i, *s: (0, index(i), 0))

    def plane(index):
        return pl.BlockSpec((ROWS, width), lambda i, *s: (index(i), 0))

    parcel_shape = jax.ShapeDtypeStruct((2 * blocks, PARCEL, LANES), jnp.float32)
    parts_shape = pltpu.VMEM((6, levels, ROWS, width), jnp.float32)
    in_smem = pl.BlockSpec(memory_space=pltpu.SMEM)
    here, after = (lambda i: i), (lambda i: i + 1)
    parcels = pl.pallas_call(
        early_kernel,
        grid=(blocks - 1,),
        in_specs=[
            field(here),
            field(after),
            field(here),
            in_smem,
            plane(here),
            plane(here),
            plane(here),
            plane(here),
            plane(after),
            plane(here),
        ],
        out_specs=pl.BlockSpec((2, PARCEL, LANES), lambda i: (i, 0, 0)),
        out_shape=parcel_shape,
        scratch_shapes=[parts_shape],
        cost_estimate=pl.CostEstimate(
            flops=8_000_000_000, bytes_accessed=4_000_000, transcendentals=0
        ),
        name="early_rows",
    )(
        theta_field,
        theta_field,
        meridional_speed,
        tier_vertical_span,
        grid_zonal_span,
        grid_plan_extent,
        ocean_energy_input,
        ocean_tier_tally,
        ocean_tier_tally,
        grid_region_label,
    )
    final = lambda i: blocks - 1
    whole = lambda *shape: pl.BlockSpec(shape, lambda i, s: (0,) * len(shape))
    parcels = pl.pallas_call(
        late_kernel,
        grid_spec=pltpu.PrefetchScalarGridSpec(
            num_scalar_prefetch=1,
            grid=(1,),
            in_specs=[
                field(final),
                field(final),
                in_smem,
                plane(final),
                plane(final),
                plane(final),
                plane(final),
                plane(final),
                whole(EDGE, width),
                pl.BlockSpec((1, EDGE, width), lambda i, s: (s[0], 0, 0)),
                pl.BlockSpec((1, EDGE, width), lambda i, s: (s[1], 0, 0)),
                whole(lat_size, LANES),
                pl.BlockSpec(memory_space=pl.ANY),
            ],
            out_specs=pl.BlockSpec((2, PARCEL, LANES), lambda i, s: (blocks - 1, 0, 0)),
            scratch_shapes=[parts_shape, pltpu.VMEM((EDGE, width), jnp.float32)],
        ),
        out_shape=parcel_shape,
        input_output_aliases={13: 0},
        cost_estimate=pl.CostEstimate(
            flops=1_000_000_000, bytes_accessed=600_000, transcendentals=0
        ),
        name="late_rows",
    )(
        where_to,
        theta_field,
        meridional_speed,
        tier_vertical_span,
        grid_zonal_span,
        grid_plan_extent,
        ocean_energy_input,
        ocean_tier_tally,
        grid_region_label,
        halo,
        fold,
        fold,
        south,
        parcels,
    )
    own = jnp.sum(exchanged(parcels, "lon"), axis=0)
    everyone = exchanged(copies(own, "lon"), "lon")
    return pl.pallas_call(
        functools.partial(finish_kernel, unit_scale, implied_scale),
        out_shape=(
            jax.ShapeDtypeStruct((OCEAN_REGIONS, parallels, THERMAL_BINS), jnp.float32),
            jax.ShapeDtypeStruct((OCEAN_REGIONS, parallels, levels), jnp.float32),
            jax.ShapeDtypeStruct((OCEAN_REGIONS, parallels), jnp.float32),
            jax.ShapeDtypeStruct((OCEAN_REGIONS, parallels), jnp.float32),
        ),
        name="finish_rows",
    )(everyone)


def solution(mesh):
    in_specs = (
        P(None, "lat", "lon"),
        P(None, "lat", "lon"),
        P(),
        P("lat", "lon"),
        P("lat", "lon"),
        P("lat", "lon"),
        P("lat", "lon"),
        P("lat", "lon"),
        P("lon"),
    )
    out_specs = (P(None, "lat", None), P(None, "lat", None), P(None, "lat"), P(None, "lat"))
    return jax.shard_map(body, mesh=mesh, in_specs=in_specs, out_specs=out_specs, check_vma=False)
```

```python
import functools
import math

import jax
import jax.numpy as jnp
from jax import lax
from jax.experimental import pallas as pl
from jax.experimental.pallas import tpu as pltpu
from jax.sharding import PartitionSpec as P

THERMAL_BINS = 128
OCEAN_REGIONS = 4
THERMAL_FLOOR = -2.0
THERMAL_RANGE = 32.0

ROWS = 8
CHUNK = 16
LOW = 8
HIGH = THERMAL_BINS // LOW
GROUPS = OCEAN_REGIONS * HIGH
LANES = 128
EDGE = 24
TERMS, DEPTHS, TOTALS, EDGES, PARCEL = 16, 20, 22, 24, 56
LAST, LAST_TERMS, SHARE = 20, 24, 32
LAST_THETA, LAST_VOLUME, LAST_SPEED, LAST_DEPTH, LAST_LABEL, LAST_ROWS = 0, 16, 32, 48, 49, 56
HEAT, FLUX, MEAN, WET = 64, 68, 76, 77


def split_in_two(x):
    high = x.astype(jnp.bfloat16).astype(jnp.float32)
    return high, x - high


def over_longitude(x):
    return jnp.sum(x, axis=1, keepdims=True)


def interpolation(face, transport, basin_base):
    per_bin = THERMAL_BINS / THERMAL_RANGE
    position = jnp.clip((face - THERMAL_FLOOR) * per_bin, 0.0, THERMAL_BINS - 1.0)
    low_bin = jnp.minimum(jnp.floor(position), THERMAL_BINS - 2.0)
    digit = jnp.floor(low_bin * (1.0 / LOW))
    weighted = transport * (position - low_bin)
    return (
        basin_base + digit,
        low_bin - LOW * digit,
        *split_in_two(transport),
        *split_in_two(weighted),
    )


class Products:
    def __init__(self, width):
        packed_id = lax.broadcasted_iota(jnp.int32, (16, width), 0)
        as_packed = lambda x: x.astype(jnp.float32).astype(jnp.bfloat16)
        self.group_ids = [as_packed(packed_id + 16 * t) for t in range(GROUPS // 16)]
        self.low_ids = as_packed(packed_id & (LOW - 1))
        self.one = jnp.ones((16, width), jnp.bfloat16)
        self.none = jnp.zeros((16, width), jnp.bfloat16)
        self.width = width

    def row(self, spread, levels):
        values, groups = [], []
        for k in range(levels):
            group = spread(0, k, 16).astype(jnp.bfloat16)
            groups.append(
                jnp.concatenate(
                    [jnp.where(group == g, self.one, self.none) for g in self.group_ids], axis=0
                )
            )
            at_low = spread(1, k, 16).astype(jnp.bfloat16) == self.low_ids
            values.append(
                jnp.concatenate(
                    [
                        jnp.where(
                            at_low,
                            jnp.concatenate([spread(q, k, 8), spread(q + 1, k, 8)], axis=0).astype(
                                jnp.bfloat16
                            ),
                            self.none,
                        )
                        for q in (2, 4)
                    ],
                    axis=0,
                )
            )
        return lax.dot_general(
            jnp.concatenate(values, axis=1),
            jnp.concatenate(groups, axis=1),
            (((1,), (1,)), ((), ())),
            preferred_element_type=jnp.float32,
        )


def class_tile(first, second):
    both = jnp.concatenate([first, second], axis=1)
    plain = both[0:8] + both[8:16]
    upper = both[16:24] + both[24:32]
    moved = pltpu.roll(upper, 1, 0)
    low_id = lax.broadcasted_iota(jnp.int32, (LOW, LANES), 0)
    moved = jnp.where(low_id == 0, pltpu.roll(moved, 1, 1), moved)
    return plain - upper + moved


def rows_kernel(
    theta_hbm,
    speed_hbm,
    tier,
    zonal_hbm,
    plan_hbm,
    energy_hbm,
    depth_hbm,
    label_hbm,
    parcel,
    last,
    theta,
    speed,
    zonal,
    plan,
    energy,
    depth,
    label,
    even,
    odd,
    field_sems,
    plane_sems,
):
    levels, parallels, width = theta.shape
    blocks = parallels // ROWS
    chunks = parallels // CHUNK

    def field_copy(which, c):
        source, target = ((theta_hbm, theta), (speed_hbm, speed))[which]
        rows = pl.ds(c * CHUNK, CHUNK)
        return pltpu.make_async_copy(
            source.at[:, rows, :], target.at[:, rows, :], field_sems.at[which, c]
        )

    planes = [
        pltpu.make_async_copy(s, t, plane_sems.at[n])
        for n, (s, t) in enumerate(
            (
                (depth_hbm, depth),
                (zonal_hbm, zonal),
                (label_hbm, label),
                (energy_hbm, energy),
                (plan_hbm, plan),
            )
        )
    ]
    field_copy(0, 0).start()
    for copy in planes:
        copy.start()
    field_copy(1, 0).start()
    for c in range(1, chunks):
        field_copy(0, c).start()
        field_copy(1, c).start()

    row_id = lax.broadcasted_iota(jnp.int32, (ROWS, width), 0)
    last_row = row_id == ROWS - 1
    lane = lax.broadcasted_iota(jnp.int32, (ROWS, LANES), 1)

    def northern(own, beyond):
        return jnp.where(last_row, jnp.broadcast_to(beyond, own.shape), pltpu.roll(own, ROWS - 1, 0))

    class Block:
        def __init__(self, block, parts):
            self.block, self.parts = block, parts
            self.rows = pl.ds(pl.multiple_of(block * ROWS, ROWS), ROWS)
            ahead = jnp.minimum(block + 1, blocks - 1) * ROWS
            self.beyond = pl.ds(pl.multiple_of(ahead, ROWS), ROWS)
            own_depth = depth[self.rows, :].astype(jnp.float32)
            next_depth = depth[self.beyond, :][0:1].astype(jnp.float32)
            next_depth = jnp.where(block == blocks - 1, 0.0, next_depth)
            self.face_depth = jnp.minimum(own_depth, northern(own_depth, next_depth))
            basin = label[self.rows, :]
            self.basin_base = basin.astype(jnp.float32) * float(HIGH)
            self.in_basin = [basin == b for b in range(OCEAN_REGIONS)]
            self.span = zonal[self.rows, :]
            self.flux = energy[self.rows, :] * plan[self.rows, :]
            self.terms = jnp.zeros((ROWS, LANES), jnp.float32)
            self.running = [jnp.zeros((ROWS, 1), jnp.float32) for _ in range(OCEAN_REGIONS)]
            self.mean_sum = jnp.zeros((ROWS, width), jnp.float32)
            self.wet_sum = jnp.zeros((ROWS, width), jnp.float32)
            self.heat_sum = jnp.zeros((ROWS, width), jnp.float32)

        def level(self, k):
            own = theta[k, self.rows, :]
            face = 0.5 * (own + northern(own, theta[k, self.beyond, :][0:1]))
            volume = jnp.where(self.face_depth > float(k), tier[k] * self.span, 0.0)
            transport = volume * speed[k, self.rows, :]
            for q, value in enumerate(interpolation(face, transport, self.basin_base)):
                self.parts[q, k] = value
            self.mean_sum += volume * face
            self.wet_sum += volume
            self.heat_sum += transport * face
            for b in range(OCEAN_REGIONS):
                self.running[b] += over_longitude(jnp.where(self.in_basin[b], transport, 0.0))
                self.terms = jnp.where(lane == b * levels + k, self.running[b], self.terms)

        def close(self):
            terms = self.terms
            for b in range(OCEAN_REGIONS):
                here = self.in_basin[b]
                heat = over_longitude(jnp.where(here, self.heat_sum, 0.0))
                terms = jnp.where(lane == HEAT + b, heat, terms)
                flux = over_longitude(jnp.where(here, self.flux, 0.0))
                terms = jnp.where(lane == FLUX + b, flux, terms)
            terms = jnp.where(lane == MEAN, over_longitude(self.mean_sum), terms)
            terms = jnp.where(lane == WET, over_longitude(self.wet_sum), terms)
            parcel[2 * self.block, TERMS : TERMS + 8, :] = terms
            parcel[2 * self.block + 1, TERMS : TERMS + 8, :] = pltpu.roll(terms, 4, 0)

    products = Products(width)

    def rows_of(parts, block, fill):
        sums = []
        for r in range(ROWS):
            spread = lambda q, k, count: jnp.broadcast_to(
                parts[q, k, r : r + 1, :], (count, width)
            )
            sums.append(products.row(spread, levels))
            for k in range(r * levels // ROWS, (r + 1) * levels // ROWS):
                fill.level(k)
        for pair in range(ROWS // 2):
            parcel[2 * block + pair // 2, 8 * (pair % 2) : 8 * (pair % 2) + 8, :] = class_tile(
                sums[2 * pair], sums[2 * pair + 1]
            )
        fill.close()

    for copy in planes:
        copy.wait()
    field_copy(0, 0).wait()
    field_copy(1, 0).wait()
    opening = Block(jnp.int32(0), even)
    for k in range(levels):
        opening.level(k)
    opening.close()

    def two_blocks(i, carry):
        @pl.when(i < chunks - 1)
        def _():
            field_copy(0, i + 1).wait()
            field_copy(1, i + 1).wait()

        rows_of(even, 2 * i, Block(2 * i + 1, odd))
        rows_of(odd, 2 * i + 1, Block(jnp.minimum(2 * i + 2, blocks - 1), even))
        return carry

    lax.fori_loop(0, chunks, two_blocks, 0)

    final = parallels - 1
    half = width // 2
    span = zonal[final : final + 1, :]
    for k in range(levels):
        last[LAST_THETA + k : LAST_THETA + k + 1, :] = theta[k, final : final + 1, :]
        last[LAST_VOLUME + k : LAST_VOLUME + k + 1, :] = tier[k] * span
        last[LAST_SPEED + k : LAST_SPEED + k + 1, :] = speed[k, final : final + 1, :]
    north_depth = depth[final : final + 1, :].astype(jnp.float32)
    last[LAST_DEPTH : LAST_DEPTH + 1, :] = north_depth
    last[LAST_LABEL : LAST_LABEL + 1, :] = label[final : final + 1, :].astype(jnp.float32)
    last[LAST_LABEL + 1 :, :] = jnp.zeros((LAST_ROWS - LAST_LABEL - 1, width), jnp.float32)
    totals = jnp.zeros((ROWS, LANES), jnp.float32)
    for d in range(0, 2 * blocks, 2):
        totals = totals + parcel[d, TERMS : TERMS + 8, :]
    totals = jnp.sum(totals, axis=0, keepdims=True)
    north = last[LAST_THETA : LAST_THETA + levels, :]
    for d in range(2 * blocks):
        parcel[d, DEPTHS : DEPTHS + 1, :] = north_depth[:, :half]
        parcel[d, DEPTHS + 1 : DEPTHS + 2, :] = north_depth[:, half:]
        parcel[d, TOTALS : TOTALS + 1, :] = totals
        parcel[d, TOTALS + 1 : TOTALS + 2, :] = jnp.zeros((1, LANES), jnp.float32)
        parcel[d, EDGES : EDGES + levels, :] = north[:, :half]
        parcel[d, EDGES + levels : EDGES + 2 * levels, :] = north[:, half:]


def last_kernel(where_to, parcels, last, halo, share, parts, edge):
    levels = EDGE - 8
    width = last.shape[1]
    devices = parcels.shape[0]
    total = parcels[0, 0:EDGES, :]
    for d in range(1, devices):
        total = total + parcels[d, 0:EDGES, :]
    columns = []
    for n in range(2):
        source = where_to[n]
        for h in range(2):
            columns.append(
                jnp.concatenate(
                    [
                        parcels[source, EDGES + h * levels : EDGES + (h + 1) * levels, :],
                        parcels[source, DEPTHS + h : DEPTHS + h + 1, :],
                        jnp.zeros((EDGE - levels - 1, LANES), jnp.float32),
                    ],
                    axis=0,
                )
            )
    columns = jnp.concatenate(columns, axis=1)
    high, rest = split_in_two(columns)
    middle, lowest = split_in_two(rest)
    source = lax.broadcasted_iota(jnp.int32, (2 * width, width), 0)
    target = lax.broadcasted_iota(jnp.int32, (2 * width, width), 1)
    mirror = jnp.where(source + target == where_to[2] + (width - 1), 1.0, 0.0).astype(jnp.bfloat16)
    pieces = jnp.dot(
        jnp.concatenate([high, middle, lowest], axis=0).astype(jnp.bfloat16),
        mirror,
        preferred_element_type=jnp.float32,
    )
    folded = pieces[0:EDGE] + pieces[EDGE : 2 * EDGE] + pieces[2 * EDGE : 3 * EDGE]
    edge[...] = jnp.where(where_to[3] == 1, folded, halo[...])

    own = last[LAST_THETA : LAST_THETA + levels, :]
    face = 0.5 * (own + edge[0:levels, :])
    face_depth = jnp.minimum(last[LAST_DEPTH : LAST_DEPTH + 1, :], edge[levels : levels + 1, :])
    level_id = lax.broadcasted_iota(jnp.int32, own.shape, 0).astype(jnp.float32)
    volume = jnp.where(
        level_id < jnp.broadcast_to(face_depth, own.shape),
        last[LAST_VOLUME : LAST_VOLUME + levels, :],
        0.0,
    )
    transport = volume * last[LAST_SPEED : LAST_SPEED + levels, :]
    basin = jnp.broadcast_to(last[LAST_LABEL : LAST_LABEL + 1, :], own.shape)
    for q, value in enumerate(interpolation(face, transport, basin * float(HIGH))):
        parts[q] = value
    sums = Products(width).row(
        lambda q, k, count: jnp.broadcast_to(parts[q, k : k + 1, :], (count, width)), levels
    )
    last_class = class_tile(sums, jnp.zeros_like(sums))

    lane = lax.broadcasted_iota(jnp.int32, (levels, LANES), 1)
    below = lax.broadcasted_iota(jnp.int32, (levels, LANES), 0) <= lane % levels
    heat = transport * face
    everything = lambda x: over_longitude(jnp.sum(x, axis=0, keepdims=True))
    running = jnp.zeros((levels, LANES), jnp.float32)
    lane1 = lane[0:1]
    terms = jnp.zeros((1, LANES), jnp.float32)
    for b in range(OCEAN_REGIONS):
        here = basin == float(b)
        level_sum = over_longitude(jnp.where(here, transport, 0.0))
        running = jnp.where((lane // levels == b) & below, level_sum, running)
        terms = jnp.where(lane1 == HEAT + b, everything(jnp.where(here, heat, 0.0)), terms)
    terms = jnp.where(lane1 == MEAN, everything(volume * face), terms)
    terms = jnp.where(lane1 == WET, everything(volume), terms)
    terms = terms + jnp.sum(running, axis=0, keepdims=True)

    place_id = lax.broadcasted_iota(jnp.int32, (EDGE, LANES), 0)
    lane24 = lax.broadcasted_iota(jnp.int32, (EDGE, LANES), 1)
    wanted = jnp.where(
        place_id < 16, (place_id & 1) * OCEAN_REGIONS + (place_id >> 2), place_id - 16
    )
    of_place = wanted == (lane24 >> 4)
    from_pair = jnp.where(place_id < 16, (place_id >> 1) & 1, 2)
    tiles = (total[0:8], total[8:16], last_class)
    wide = []
    for low in range(LOW):
        row = jnp.zeros((EDGE, LANES), jnp.float32)
        for n, tile in enumerate(tiles):
            row = jnp.where(
                of_place & (from_pair == n),
                jnp.broadcast_to(tile[low : low + 1], (EDGE, LANES)),
                row,
            )
        wide.append(row)
    wide_high, wide_low = split_in_two(jnp.concatenate(wide, axis=1))
    from_id = lax.broadcasted_iota(jnp.int32, (LANES, LANES), 0)
    to_id = lax.broadcasted_iota(jnp.int32, (LANES, LANES), 1)
    goal = (from_id & (HIGH - 1)) * LOW
    placing = jnp.concatenate(
        [jnp.where(to_id == goal + low, 1.0, 0.0) for low in range(LOW)], axis=0
    ).astype(jnp.bfloat16)
    placed = jnp.dot(
        jnp.concatenate([wide_high, wide_low], axis=0).astype(jnp.bfloat16),
        placing,
        preferred_element_type=jnp.float32,
    )
    placed = placed[0:EDGE] + placed[EDGE : 2 * EDGE]
    share[0:16, :] = placed[0:16]
    share[TERMS : TERMS + 4, :] = total[TERMS : TERMS + 4]
    share[LAST : LAST + 4, :] = placed[16:20]
    share[LAST_TERMS : LAST_TERMS + 1, :] = terms
    share[LAST_TERMS + 1 :, :] = jnp.zeros((SHARE - LAST_TERMS - 1, LANES), jnp.float32)


def finish_kernel(unit_scale, implied_scale, where_to, shares, class_out, stream, heat, implied):
    devices = shares.shape[0]
    rows = 4 * devices
    levels = stream.shape[1]
    mine = shares[0, LAST:SHARE, :]
    for d in range(1, devices):
        mine = mine + shares[d, LAST:SHARE, :]
    for b in range(OCEAN_REGIONS):
        for d in range(devices):
            class_out[b, 4 * d : 4 * d + 4, :] = unit_scale * shares[d, 4 * b : 4 * b + 4, :]
        class_out[b, rows - 1 : rows, :] += unit_scale * mine[b : b + 1]
    terms = jnp.concatenate([shares[d, TERMS : TERMS + 4, :] for d in range(devices)], axis=0)
    row_id = lax.broadcasted_iota(jnp.int32, terms.shape, 0)
    own_terms = mine[LAST_TERMS - LAST : LAST_TERMS - LAST + 1]
    terms = terms + jnp.where(row_id == rows - 1, jnp.broadcast_to(own_terms, terms.shape), 0.0)
    turned = jnp.transpose(
        jnp.concatenate([terms, jnp.zeros((LANES - rows, LANES), jnp.float32)], axis=0)
    )
    for b in range(OCEAN_REGIONS):
        stream[b] = unit_scale * turned[b * levels : (b + 1) * levels, :rows]
    lane = lax.broadcasted_iota(jnp.int32, (1, LANES), 1)
    row_mean = turned[MEAN : MEAN + 1] / jnp.where(lane < rows, turned[WET : WET + 1], 1.0)
    offsets = jnp.zeros((1, LANES), jnp.float32)
    for d in range(devices):
        offsets += jnp.where(d < where_to[4], shares[d, SHARE - 1 : SHARE, :], 0.0)
    for b in range(OCEAN_REGIONS):
        total = turned[(b + 1) * levels - 1 : (b + 1) * levels]
        out = unit_scale / 16.0 * (turned[HEAT + b : HEAT + b + 1] - total * row_mean)
        heat[b : b + 1, :] = out[:, :rows]
        flux = turned[FLUX + b : FLUX + b + 1]
        offset = over_longitude(jnp.where(lane == FLUX + b, offsets, 0.0))
        shift = 1
        while shift < rows:
            flux = flux + jnp.where(lane >= shift, pltpu.roll(flux, shift, 1), 0.0)
            shift *= 2
        implied[b : b + 1, :] = (implied_scale * (flux + offset))[:, :rows]


def exchanged(pieces, axis):
    return lax.all_to_all(pieces, axis, split_axis=0, concat_axis=0, tiled=True)


def body(
    meridional_speed,
    theta_field,
    tier_vertical_span,
    grid_zonal_span,
    grid_plan_extent,
    ocean_energy_input,
    ocean_tier_tally,
    grid_region_label,
    seam_matching_meridian,
):
    levels, parallels, width = theta_field.shape
    lon_size = lax.axis_size("lon")
    lat_size = lax.axis_size("lat")
    lat_index = lax.axis_index("lat")
    width_total = width * lon_size
    unit_scale = math.sqrt(THERMAL_BINS / (width_total * levels))
    implied_scale = 2.0 / math.sqrt(width_total * parallels * lat_size)
    blocks = parallels // ROWS
    chunks = parallels // CHUNK

    southernmost = jnp.concatenate(
        [
            theta_field[:, 0, :],
            ocean_tier_tally[0][None].astype(jnp.float32),
            jnp.zeros((EDGE - levels - 1, width), jnp.float32),
        ]
    )
    halo = lax.ppermute(southernmost, "lat", [(i + 1, i) for i in range(lat_size - 1)])

    start = (seam_matching_meridian[0] + (width_total - (width - 1))) % width_total
    first = start // width
    where_to = jnp.stack(
        [
            first,
            (first + 1) % lon_size,
            start % width,
            (lat_index == lat_size - 1).astype(jnp.int32),
            lat_index.astype(jnp.int32),
        ]
    )

    in_smem = pl.BlockSpec(memory_space=pltpu.SMEM)
    in_vmem = pl.BlockSpec(memory_space=pltpu.VMEM)
    anywhere = pl.BlockSpec(memory_space=pl.ANY)
    plane_f32 = pltpu.VMEM((parallels, width), jnp.float32)
    plane_i32 = pltpu.VMEM((parallels, width), jnp.int32)
    field = pltpu.VMEM((levels, parallels, width), jnp.float32)
    parts = pltpu.VMEM((6, levels, ROWS, width), jnp.float32)
    parcels, last = pl.pallas_call(
        rows_kernel,
        in_specs=[anywhere, anywhere, in_smem] + [anywhere] * 5,
        out_specs=(in_vmem, in_vmem),
        out_shape=(
            jax.ShapeDtypeStruct((2 * blocks, PARCEL, LANES), jnp.float32),
            jax.ShapeDtypeStruct((LAST_ROWS, width), jnp.float32),
        ),
        scratch_shapes=[
            field,
            field,
            plane_f32,
            plane_f32,
            plane_f32,
            plane_i32,
            plane_i32,
            parts,
            parts,
            pltpu.SemaphoreType.DMA((2, chunks)),
            pltpu.SemaphoreType.DMA((5,)),
        ],
        cost_estimate=pl.CostEstimate(
            flops=8_000_000_000, bytes_accessed=4_000_000, transcendentals=0
        ),
        name="rows",
    )(
        theta_field,
        meridional_speed,
        tier_vertical_span,
        grid_zonal_span,
        grid_plan_extent,
        ocean_energy_input,
        ocean_tier_tally,
        grid_region_label,
    )
    received = exchanged(parcels, "lon")
    row_flux = jnp.sum(received[:, TOTALS, :], axis=0)[None]
    turned = [
        (s * lon_size + r, r * lon_size + s) for s in range(lat_size) for r in range(lon_size)
    ]
    of_block = lax.ppermute(row_flux, ("lon", "lat"), turned)
    share = pl.pallas_call(
        last_kernel,
        in_specs=[in_smem, in_vmem, in_vmem, in_vmem],
        out_specs=in_vmem,
        out_shape=jax.ShapeDtypeStruct((SHARE, LANES), jnp.float32),
        scratch_shapes=[
            pltpu.VMEM((6, levels, width), jnp.float32),
            pltpu.VMEM((EDGE, width), jnp.float32),
        ],
        cost_estimate=pl.CostEstimate(
            flops=1_000_000_000, bytes_accessed=600_000, transcendentals=0
        ),
        name="last_row",
    )(where_to, received, last, halo)
    share = jnp.concatenate([share[: SHARE - 1], of_block])
    shares = exchanged(jnp.broadcast_to(share, (lon_size, SHARE, LANES)), "lon")
    class_out, stream, heat, implied = pl.pallas_call(
        functools.partial(finish_kernel, unit_scale, implied_scale),
        in_specs=[in_smem, in_vmem],
        out_specs=(in_vmem,) * 4,
        out_shape=(
            jax.ShapeDtypeStruct((OCEAN_REGIONS, parallels, THERMAL_BINS), jnp.float32),
            jax.ShapeDtypeStruct((OCEAN_REGIONS, levels, parallels), jnp.float32),
            jax.ShapeDtypeStruct((OCEAN_REGIONS, parallels), jnp.float32),
            jax.ShapeDtypeStruct((OCEAN_REGIONS, parallels), jnp.float32),
        ),
        name="finish",
    )(where_to, shares)
    return class_out, jnp.transpose(stream, (0, 2, 1)), heat, implied


def solution(mesh):
    in_specs = (
        P(None, "lat", "lon"),
        P(None, "lat", "lon"),
        P(),
        P("lat", "lon"),
        P("lat", "lon"),
        P("lat", "lon"),
        P("lat", "lon"),
        P("lat", "lon"),
        P("lon"),
    )
    out_specs = (P(None, "lat", None), P(None, "lat", None), P(None, "lat"), P(None, "lat"))
    return jax.shard_map(body, mesh=mesh, in_specs=in_specs, out_specs=out_specs, check_vma=False)
```

```python
import functools
import math

import jax
import jax.numpy as jnp
from jax import lax
from jax.experimental import pallas as pl
from jax.experimental.pallas import tpu as pltpu
from jax.sharding import PartitionSpec as P

THERMAL_BINS = 128
OCEAN_REGIONS = 4
THERMAL_FLOOR = -2.0
THERMAL_RANGE = 32.0

ROWS = 8
CHUNK = 16
LOW = 8
HIGH = THERMAL_BINS // LOW
GROUPS = OCEAN_REGIONS * HIGH
LANES = 128
EDGE = 24
TERMS, DEPTHS, TOTALS, EDGES, PARCEL = 16, 20, 22, 24, 56
LAST, LAST_TERMS, SHARE = 20, 24, 32
LAST_THETA, LAST_VOLUME, LAST_SPEED, LAST_DEPTH, LAST_LABEL, LAST_ROWS = 0, 16, 32, 48, 49, 56
HEAT, FLUX, MEAN, WET = 64, 68, 76, 77


def split_in_two(x):
    high = x.astype(jnp.bfloat16).astype(jnp.float32)
    return high, x - high


def over_longitude(x):
    return jnp.sum(x, axis=1, keepdims=True)


def interpolation(face, transport, basin_base):
    per_bin = THERMAL_BINS / THERMAL_RANGE
    position = jnp.clip((face - THERMAL_FLOOR) * per_bin, 0.0, THERMAL_BINS - 1.0)
    low_bin = jnp.minimum(jnp.floor(position), THERMAL_BINS - 2.0)
    digit = jnp.floor(low_bin * (1.0 / LOW))
    weighted = transport * (position - low_bin)
    return (
        basin_base + digit,
        low_bin - LOW * digit,
        *split_in_two(transport),
        *split_in_two(weighted),
    )


class Products:
    def __init__(self, width):
        packed_id = lax.broadcasted_iota(jnp.int32, (16, width), 0)
        as_packed = lambda x: x.astype(jnp.float32).astype(jnp.bfloat16)
        self.group_ids = [as_packed(packed_id + 16 * t) for t in range(GROUPS // 16)]
        self.low_ids = as_packed(packed_id & (LOW - 1))
        self.one = jnp.ones((16, width), jnp.bfloat16)
        self.none = jnp.zeros((16, width), jnp.bfloat16)
        self.width = width

    def row(self, spread, levels):
        values, groups = [], []
        for k in range(levels):
            group = spread(0, k, 16).astype(jnp.bfloat16)
            groups.append(
                jnp.concatenate(
                    [jnp.where(group == g, self.one, self.none) for g in self.group_ids], axis=0
                )
            )
            at_low = spread(1, k, 16).astype(jnp.bfloat16) == self.low_ids
            values.append(
                jnp.concatenate(
                    [
                        jnp.where(
                            at_low,
                            jnp.concatenate([spread(q, k, 8), spread(q + 1, k, 8)], axis=0).astype(
                                jnp.bfloat16
                            ),
                            self.none,
                        )
                        for q in (2, 4)
                    ],
                    axis=0,
                )
            )
        return lax.dot_general(
            jnp.concatenate(values, axis=1),
            jnp.concatenate(groups, axis=1),
            (((1,), (1,)), ((), ())),
            preferred_element_type=jnp.float32,
        )


def class_tile(first, second):
    both = jnp.concatenate([first, second], axis=1)
    plain = both[0:8] + both[8:16]
    upper = both[16:24] + both[24:32]
    moved = pltpu.roll(upper, 1, 0)
    low_id = lax.broadcasted_iota(jnp.int32, (LOW, LANES), 0)
    moved = jnp.where(low_id == 0, pltpu.roll(moved, 1, 1), moved)
    return plain - upper + moved


def rows_kernel(
    theta_hbm,
    speed_hbm,
    tier,
    zonal_hbm,
    plan_hbm,
    energy_hbm,
    depth_hbm,
    label_hbm,
    parcel,
    last,
    theta,
    speed,
    zonal,
    plan,
    energy,
    depth,
    label,
    even,
    odd,
    field_sems,
    plane_sems,
):
    levels, parallels, width = theta.shape
    blocks = parallels // ROWS
    chunks = parallels // CHUNK

    def field_copy(which, c):
        source, target = ((theta_hbm, theta), (speed_hbm, speed))[which]
        rows = pl.ds(c * CHUNK, CHUNK)
        return pltpu.make_async_copy(
            source.at[:, rows, :], target.at[:, rows, :], field_sems.at[which, c]
        )

    planes = [
        pltpu.make_async_copy(s, t, plane_sems.at[n])
        for n, (s, t) in enumerate(
            (
                (depth_hbm, depth),
                (zonal_hbm, zonal),
                (label_hbm, label),
                (energy_hbm, energy),
                (plan_hbm, plan),
            )
        )
    ]
    field_copy(0, 0).start()
    for copy in planes:
        copy.start()
    field_copy(1, 0).start()
    for c in range(1, chunks):
        field_copy(0, c).start()
        field_copy(1, c).start()

    row_id = lax.broadcasted_iota(jnp.int32, (ROWS, width), 0)
    last_row = row_id == ROWS - 1
    lane = lax.broadcasted_iota(jnp.int32, (ROWS, LANES), 1)

    def northern(own, beyond):
        return jnp.where(last_row, jnp.broadcast_to(beyond, own.shape), pltpu.roll(own, ROWS - 1, 0))

    class Block:
        def __init__(self, block, parts):
            self.block, self.parts = block, parts
            self.rows = pl.ds(pl.multiple_of(block * ROWS, ROWS), ROWS)
            ahead = jnp.minimum(block + 1, blocks - 1) * ROWS
            self.beyond = pl.ds(pl.multiple_of(ahead, ROWS), ROWS)
            own_depth = depth[self.rows, :].astype(jnp.float32)
            next_depth = depth[self.beyond, :][0:1].astype(jnp.float32)
            next_depth = jnp.where(block == blocks - 1, 0.0, next_depth)
            self.face_depth = jnp.minimum(own_depth, northern(own_depth, next_depth))
            basin = label[self.rows, :]
            self.basin_base = basin.astype(jnp.float32) * float(HIGH)
            self.in_basin = [basin == b for b in range(OCEAN_REGIONS)]
            self.span = zonal[self.rows, :]
            self.flux = energy[self.rows, :] * plan[self.rows, :]
            self.terms = jnp.zeros((ROWS, LANES), jnp.float32)
            self.running = [jnp.zeros((ROWS, 1), jnp.float32) for _ in range(OCEAN_REGIONS)]
            self.mean_sum = jnp.zeros((ROWS, width), jnp.float32)
            self.wet_sum = jnp.zeros((ROWS, width), jnp.float32)
            self.heat_sum = jnp.zeros((ROWS, width), jnp.float32)

        def level(self, k):
            own = theta[k, self.rows, :]
            face = 0.5 * (own + northern(own, theta[k, self.beyond, :][0:1]))
            volume = jnp.where(self.face_depth > float(k), tier[k] * self.span, 0.0)
            transport = volume * speed[k, self.rows, :]
            for q, value in enumerate(interpolation(face, transport, self.basin_base)):
                self.parts[q, k] = value
            self.mean_sum += volume * face
            self.wet_sum += volume
            self.heat_sum += transport * face
            for b in range(OCEAN_REGIONS):
                self.running[b] += over_longitude(jnp.where(self.in_basin[b], transport, 0.0))
                self.terms = jnp.where(lane == b * levels + k, self.running[b], self.terms)

        def close(self):
            terms = self.terms
            for b in range(OCEAN_REGIONS):
                here = self.in_basin[b]
                heat = over_longitude(jnp.where(here, self.heat_sum, 0.0))
                terms = jnp.where(lane == HEAT + b, heat, terms)
                flux = over_longitude(jnp.where(here, self.flux, 0.0))
                terms = jnp.where(lane == FLUX + b, flux, terms)
            terms = jnp.where(lane == MEAN, over_longitude(self.mean_sum), terms)
            terms = jnp.where(lane == WET, over_longitude(self.wet_sum), terms)
            parcel[2 * self.block, TERMS : TERMS + 8, :] = terms
            parcel[2 * self.block + 1, TERMS : TERMS + 8, :] = pltpu.roll(terms, 4, 0)

    products = Products(width)

    def rows_of(parts, block, fill):
        sums = []
        for r in range(ROWS):
            spread = lambda q, k, count: jnp.broadcast_to(
                parts[q, k, r : r + 1, :], (count, width)
            )
            sums.append(products.row(spread, levels))
            for k in range(r * levels // ROWS, (r + 1) * levels // ROWS):
                fill.level(k)
        for pair in range(ROWS // 2):
            parcel[2 * block + pair // 2, 8 * (pair % 2) : 8 * (pair % 2) + 8, :] = class_tile(
                sums[2 * pair], sums[2 * pair + 1]
            )
        fill.close()

    for copy in planes:
        copy.wait()
    field_copy(0, 0).wait()
    field_copy(1, 0).wait()
    opening = Block(jnp.int32(0), even)
    for k in range(levels):
        opening.level(k)
    opening.close()

    def two_blocks(i, carry):
        @pl.when(i < chunks - 1)
        def _():
            field_copy(0, i + 1).wait()
            field_copy(1, i + 1).wait()

        rows_of(even, 2 * i, Block(2 * i + 1, odd))
        rows_of(odd, 2 * i + 1, Block(jnp.minimum(2 * i + 2, blocks - 1), even))
        return carry

    lax.fori_loop(0, chunks, two_blocks, 0)

    final = parallels - 1
    half = width // 2
    span = zonal[final : final + 1, :]
    for k in range(levels):
        last[LAST_THETA + k : LAST_THETA + k + 1, :] = theta[k, final : final + 1, :]
        last[LAST_VOLUME + k : LAST_VOLUME + k + 1, :] = tier[k] * span
        last[LAST_SPEED + k : LAST_SPEED + k + 1, :] = speed[k, final : final + 1, :]
    north_depth = depth[final : final + 1, :].astype(jnp.float32)
    last[LAST_DEPTH : LAST_DEPTH + 1, :] = north_depth
    last[LAST_LABEL : LAST_LABEL + 1, :] = label[final : final + 1, :].astype(jnp.float32)
    last[LAST_LABEL + 1 :, :] = jnp.zeros((LAST_ROWS - LAST_LABEL - 1, width), jnp.float32)
    totals = jnp.zeros((ROWS, LANES), jnp.float32)
    for d in range(0, 2 * blocks, 2):
        totals = totals + parcel[d, TERMS : TERMS + 8, :]
    totals = jnp.sum(totals, axis=0, keepdims=True)
    north = last[LAST_THETA : LAST_THETA + levels, :]
    for d in range(2 * blocks):
        parcel[d, DEPTHS : DEPTHS + 1, :] = north_depth[:, :half]
        parcel[d, DEPTHS + 1 : DEPTHS + 2, :] = north_depth[:, half:]
        parcel[d, TOTALS : TOTALS + 1, :] = totals
        parcel[d, TOTALS + 1 : TOTALS + 2, :] = jnp.zeros((1, LANES), jnp.float32)
        parcel[d, EDGES : EDGES + levels, :] = north[:, :half]
        parcel[d, EDGES + levels : EDGES + 2 * levels, :] = north[:, half:]


def last_kernel(where_to, parcels, last, halo, share, parts, edge):
    levels = EDGE - 8
    width = last.shape[1]
    devices = parcels.shape[0]
    total = parcels[0, 0:EDGES, :]
    for d in range(1, devices):
        total = total + parcels[d, 0:EDGES, :]
    columns = []
    for n in range(2):
        source = where_to[n]
        for h in range(2):
            columns.append(
                jnp.concatenate(
                    [
                        parcels[source, EDGES + h * levels : EDGES + (h + 1) * levels, :],
                        parcels[source, DEPTHS + h : DEPTHS + h + 1, :],
                        jnp.zeros((EDGE - levels - 1, LANES), jnp.float32),
                    ],
                    axis=0,
                )
            )
    columns = jnp.concatenate(columns, axis=1)
    high, rest = split_in_two(columns)
    middle, lowest = split_in_two(rest)
    source = lax.broadcasted_iota(jnp.int32, (2 * width, width), 0)
    target = lax.broadcasted_iota(jnp.int32, (2 * width, width), 1)
    mirror = jnp.where(source + target == where_to[2] + (width - 1), 1.0, 0.0).astype(jnp.bfloat16)
    pieces = jnp.dot(
        jnp.concatenate([high, middle, lowest], axis=0).astype(jnp.bfloat16),
        mirror,
        preferred_element_type=jnp.float32,
    )
    folded = pieces[0:EDGE] + pieces[EDGE : 2 * EDGE] + pieces[2 * EDGE : 3 * EDGE]
    edge[...] = jnp.where(where_to[3] == 1, folded, halo[...])

    own = last[LAST_THETA : LAST_THETA + levels, :]
    face = 0.5 * (own + edge[0:levels, :])
    face_depth = jnp.minimum(last[LAST_DEPTH : LAST_DEPTH + 1, :], edge[levels : levels + 1, :])
    level_id = lax.broadcasted_iota(jnp.int32, own.shape, 0).astype(jnp.float32)
    volume = jnp.where(
        level_id < jnp.broadcast_to(face_depth, own.shape),
        last[LAST_VOLUME : LAST_VOLUME + levels, :],
        0.0,
    )
    transport = volume * last[LAST_SPEED : LAST_SPEED + levels, :]
    basin = jnp.broadcast_to(last[LAST_LABEL : LAST_LABEL + 1, :], own.shape)
    for q, value in enumerate(interpolation(face, transport, basin * float(HIGH))):
        parts[q] = value
    sums = Products(width).row(
        lambda q, k, count: jnp.broadcast_to(parts[q, k : k + 1, :], (count, width)), levels
    )
    last_class = class_tile(sums, jnp.zeros_like(sums))

    lane = lax.broadcasted_iota(jnp.int32, (levels, LANES), 1)
    below = lax.broadcasted_iota(jnp.int32, (levels, LANES), 0) <= lane % levels
    heat = transport * face
    everything = lambda x: over_longitude(jnp.sum(x, axis=0, keepdims=True))
    running = jnp.zeros((levels, LANES), jnp.float32)
    lane1 = lane[0:1]
    terms = jnp.zeros((1, LANES), jnp.float32)
    for b in range(OCEAN_REGIONS):
        here = basin == float(b)
        level_sum = over_longitude(jnp.where(here, transport, 0.0))
        running = jnp.where((lane // levels == b) & below, level_sum, running)
        terms = jnp.where(lane1 == HEAT + b, everything(jnp.where(here, heat, 0.0)), terms)
    terms = jnp.where(lane1 == MEAN, everything(volume * face), terms)
    terms = jnp.where(lane1 == WET, everything(volume), terms)
    terms = terms + jnp.sum(running, axis=0, keepdims=True)

    place_id = lax.broadcasted_iota(jnp.int32, (EDGE, LANES), 0)
    lane24 = lax.broadcasted_iota(jnp.int32, (EDGE, LANES), 1)
    wanted = jnp.where(
        place_id < 16, (place_id & 1) * OCEAN_REGIONS + (place_id >> 2), place_id - 16
    )
    of_place = wanted == (lane24 >> 4)
    from_pair = jnp.where(place_id < 16, (place_id >> 1) & 1, 2)
    tiles = (total[0:8], total[8:16], last_class)
    wide = []
    for low in range(LOW):
        row = jnp.zeros((EDGE, LANES), jnp.float32)
        for n, tile in enumerate(tiles):
            row = jnp.where(
                of_place & (from_pair == n),
                jnp.broadcast_to(tile[low : low + 1], (EDGE, LANES)),
                row,
            )
        wide.append(row)
    wide_high, wide_low = split_in_two(jnp.concatenate(wide, axis=1))
    from_id = lax.broadcasted_iota(jnp.int32, (LANES, LANES), 0)
    to_id = lax.broadcasted_iota(jnp.int32, (LANES, LANES), 1)
    goal = (from_id & (HIGH - 1)) * LOW
    placing = jnp.concatenate(
        [jnp.where(to_id == goal + low, 1.0, 0.0) for low in range(LOW)], axis=0
    ).astype(jnp.bfloat16)
    placed = jnp.dot(
        jnp.concatenate([wide_high, wide_low], axis=0).astype(jnp.bfloat16),
        placing,
        preferred_element_type=jnp.float32,
    )
    placed = placed[0:EDGE] + placed[EDGE : 2 * EDGE]
    share[0:16, :] = placed[0:16]
    share[TERMS : TERMS + 4, :] = total[TERMS : TERMS + 4]
    share[LAST : LAST + 4, :] = placed[16:20]
    share[LAST_TERMS : LAST_TERMS + 1, :] = terms
    share[LAST_TERMS + 1 :, :] = jnp.zeros((SHARE - LAST_TERMS - 1, LANES), jnp.float32)


def finish_kernel(unit_scale, implied_scale, where_to, shares, class_out, stream, heat, implied):
    devices = shares.shape[0]
    rows = 4 * devices
    levels = stream.shape[1]
    mine = shares[0, LAST:SHARE, :]
    for d in range(1, devices):
        mine = mine + shares[d, LAST:SHARE, :]
    for b in range(OCEAN_REGIONS):
        for d in range(devices):
            class_out[b, 4 * d : 4 * d + 4, :] = unit_scale * shares[d, 4 * b : 4 * b + 4, :]
        class_out[b, rows - 1 : rows, :] += unit_scale * mine[b : b + 1]
    terms = jnp.concatenate([shares[d, TERMS : TERMS + 4, :] for d in range(devices)], axis=0)
    row_id = lax.broadcasted_iota(jnp.int32, terms.shape, 0)
    own_terms = mine[LAST_TERMS - LAST : LAST_TERMS - LAST + 1]
    terms = terms + jnp.where(row_id == rows - 1, jnp.broadcast_to(own_terms, terms.shape), 0.0)
    turned = jnp.transpose(
        jnp.concatenate([terms, jnp.zeros((LANES - rows, LANES), jnp.float32)], axis=0)
    )
    for b in range(OCEAN_REGIONS):
        stream[b] = unit_scale * turned[b * levels : (b + 1) * levels, :rows]
    lane = lax.broadcasted_iota(jnp.int32, (1, LANES), 1)
    row_mean = turned[MEAN : MEAN + 1] / jnp.where(lane < rows, turned[WET : WET + 1], 1.0)
    offsets = jnp.zeros((1, LANES), jnp.float32)
    for d in range(devices):
        offsets += shares[d, SHARE - 1 : SHARE, :]
    for b in range(OCEAN_REGIONS):
        total = turned[(b + 1) * levels - 1 : (b + 1) * levels]
        out = unit_scale / 16.0 * (turned[HEAT + b : HEAT + b + 1] - total * row_mean)
        heat[b : b + 1, :] = out[:, :rows]
        flux = turned[FLUX + b : FLUX + b + 1]
        offset = over_longitude(jnp.where(lane == FLUX + b, offsets, 0.0))
        shift = 1
        while shift < rows:
            flux = flux + jnp.where(lane >= shift, pltpu.roll(flux, shift, 1), 0.0)
            shift *= 2
        implied[b : b + 1, :] = (implied_scale * (flux + offset))[:, :rows]


def exchanged(pieces, axis):
    return lax.all_to_all(pieces, axis, split_axis=0, concat_axis=0, tiled=True)


def body(
    meridional_speed,
    theta_field,
    tier_vertical_span,
    grid_zonal_span,
    grid_plan_extent,
    ocean_energy_input,
    ocean_tier_tally,
    grid_region_label,
    seam_matching_meridian,
):
    levels, parallels, width = theta_field.shape
    lon_size = lax.axis_size("lon")
    lat_size = lax.axis_size("lat")
    lat_index = lax.axis_index("lat")
    width_total = width * lon_size
    unit_scale = math.sqrt(THERMAL_BINS / (width_total * levels))
    implied_scale = 2.0 / math.sqrt(width_total * parallels * lat_size)
    blocks = parallels // ROWS
    chunks = parallels // CHUNK

    southernmost = jnp.concatenate(
        [
            theta_field[:, 0, :],
            ocean_tier_tally[0][None].astype(jnp.float32),
            jnp.zeros((EDGE - levels - 1, width), jnp.float32),
        ]
    )
    halo = lax.ppermute(southernmost, "lat", [(i + 1, i) for i in range(lat_size - 1)])

    start = (seam_matching_meridian[0] + (width_total - (width - 1))) % width_total
    first = start // width
    where_to = jnp.stack(
        [
            first,
            (first + 1) % lon_size,
            start % width,
            (lat_index == lat_size - 1).astype(jnp.int32),
            lat_index.astype(jnp.int32),
        ]
    )

    in_smem = pl.BlockSpec(memory_space=pltpu.SMEM)
    in_vmem = pl.BlockSpec(memory_space=pltpu.VMEM)
    anywhere = pl.BlockSpec(memory_space=pl.ANY)
    plane_f32 = pltpu.VMEM((parallels, width), jnp.float32)
    plane_i32 = pltpu.VMEM((parallels, width), jnp.int32)
    field = pltpu.VMEM((levels, parallels, width), jnp.float32)
    parts = pltpu.VMEM((6, levels, ROWS, width), jnp.float32)
    parcels, last = pl.pallas_call(
        rows_kernel,
        in_specs=[anywhere, anywhere, in_smem] + [anywhere] * 5,
        out_specs=(in_vmem, in_vmem),
        out_shape=(
            jax.ShapeDtypeStruct((2 * blocks, PARCEL, LANES), jnp.float32),
            jax.ShapeDtypeStruct((LAST_ROWS, width), jnp.float32),
        ),
        scratch_shapes=[
            field,
            field,
            plane_f32,
            plane_f32,
            plane_f32,
            plane_i32,
            plane_i32,
            parts,
            parts,
            pltpu.SemaphoreType.DMA((2, chunks)),
            pltpu.SemaphoreType.DMA((5,)),
        ],
        cost_estimate=pl.CostEstimate(
            flops=8_000_000_000, bytes_accessed=4_000_000, transcendentals=0
        ),
        name="rows",
    )(
        theta_field,
        meridional_speed,
        tier_vertical_span,
        grid_zonal_span,
        grid_plan_extent,
        ocean_energy_input,
        ocean_tier_tally,
        grid_region_label,
    )
    received = exchanged(parcels, "lon")
    row_flux = jnp.sum(received[:, TOTALS, :], axis=0)[None]
    northward = [
        (r * lat_size + s, r * lat_size + s + r)
        for r in range(1, lon_size)
        for s in range(lat_size - r)
    ]
    of_block = lax.ppermute(row_flux, ("lon", "lat"), northward)
    share = pl.pallas_call(
        last_kernel,
        in_specs=[in_smem, in_vmem, in_vmem, in_vmem],
        out_specs=in_vmem,
        out_shape=jax.ShapeDtypeStruct((SHARE, LANES), jnp.float32),
        scratch_shapes=[
            pltpu.VMEM((6, levels, width), jnp.float32),
            pltpu.VMEM((EDGE, width), jnp.float32),
        ],
        cost_estimate=pl.CostEstimate(
            flops=1_000_000_000, bytes_accessed=600_000, transcendentals=0
        ),
        name="last_row",
    )(where_to, received, last, halo)
    share = jnp.concatenate([share[: SHARE - 1], of_block])
    shares = exchanged(jnp.broadcast_to(share, (lon_size, SHARE, LANES)), "lon")
    class_out, stream, heat, implied = pl.pallas_call(
        functools.partial(finish_kernel, unit_scale, implied_scale),
        in_specs=[in_smem, in_vmem],
        out_specs=(in_vmem,) * 4,
        out_shape=(
            jax.ShapeDtypeStruct((OCEAN_REGIONS, parallels, THERMAL_BINS), jnp.float32),
            jax.ShapeDtypeStruct((OCEAN_REGIONS, levels, parallels), jnp.float32),
            jax.ShapeDtypeStruct((OCEAN_REGIONS, parallels), jnp.float32),
            jax.ShapeDtypeStruct((OCEAN_REGIONS, parallels), jnp.float32),
        ),
        name="finish",
    )(where_to, shares)
    return class_out, jnp.transpose(stream, (0, 2, 1)), heat, implied


def solution(mesh):
    in_specs = (
        P(None, "lat", "lon"),
        P(None, "lat", "lon"),
        P(),
        P("lat", "lon"),
        P("lat", "lon"),
        P("lat", "lon"),
        P("lat", "lon"),
        P("lat", "lon"),
        P("lon"),
    )
    out_specs = (P(None, "lat", None), P(None, "lat", None), P(None, "lat"), P(None, "lat"))
    return jax.shard_map(body, mesh=mesh, in_specs=in_specs, out_specs=out_specs, check_vma=False)
```

```python
import functools
import math

import jax
import jax.numpy as jnp
from jax import lax
from jax.experimental import pallas as pl
from jax.experimental.pallas import tpu as pltpu
from jax.sharding import PartitionSpec as P

THERMAL_BINS = 128
OCEAN_REGIONS = 4
THERMAL_FLOOR = -2.0
THERMAL_RANGE = 32.0

ROWS = 8
CHUNK = 16
LOW = 8
HIGH = THERMAL_BINS // LOW
GROUPS = OCEAN_REGIONS * HIGH
LANES = 128
EDGE = 24
TERMS, TOTALS, LEVEL, PARCEL = 16, 20, 24, 32
BASIN_UNIT = 32.0
LAST, LAST_TERMS, SHARE = 20, 24, 32
SMALL_KERNEL = 8 * 1024 * 1024
LAST_THETA, LAST_VOLUME, LAST_SPEED, LAST_MARKS, LAST_ROWS = 0, 16, 32, 48, 56
HEAT, FLUX, MEAN, WET = 64, 68, 76, 77


def split_in_two(x):
    high = x.astype(jnp.bfloat16).astype(jnp.float32)
    return high, x - high


def over_longitude(x):
    return jnp.sum(x, axis=1, keepdims=True)


def interpolation(face, transport, basin_base):
    per_bin = THERMAL_BINS / THERMAL_RANGE
    position = jnp.clip((face - THERMAL_FLOOR) * per_bin, 0.0, THERMAL_BINS - 1.0)
    low_bin = jnp.minimum(jnp.floor(position), THERMAL_BINS - 2.0)
    digit = jnp.floor(low_bin * (1.0 / LOW))
    weighted = transport * (position - low_bin)
    return (
        basin_base + digit,
        low_bin - LOW * digit,
        *split_in_two(transport),
        *split_in_two(weighted),
    )


class Products:
    def __init__(self, width):
        packed_id = lax.broadcasted_iota(jnp.int32, (16, width), 0)
        as_packed = lambda x: x.astype(jnp.float32).astype(jnp.bfloat16)
        self.group_ids = [as_packed(packed_id + 16 * t) for t in range(GROUPS // 16)]
        self.low_ids = as_packed(packed_id & (LOW - 1))
        self.one = jnp.ones((16, width), jnp.bfloat16)
        self.none = jnp.zeros((16, width), jnp.bfloat16)
        self.width = width

    def row(self, spread, levels):
        values, groups = [], []
        for k in range(levels):
            group = spread(0, k, 16).astype(jnp.bfloat16)
            groups.append(
                jnp.concatenate(
                    [jnp.where(group == g, self.one, self.none) for g in self.group_ids], axis=0
                )
            )
            at_low = spread(1, k, 16).astype(jnp.bfloat16) == self.low_ids
            values.append(
                jnp.concatenate(
                    [
                        jnp.where(
                            at_low,
                            jnp.concatenate([spread(q, k, 8), spread(q + 1, k, 8)], axis=0).astype(
                                jnp.bfloat16
                            ),
                            self.none,
                        )
                        for q in (2, 4)
                    ],
                    axis=0,
                )
            )
        return lax.dot_general(
            jnp.concatenate(values, axis=1),
            jnp.concatenate(groups, axis=1),
            (((1,), (1,)), ((), ())),
            preferred_element_type=jnp.float32,
        )


def class_tile(first, second):
    both = jnp.concatenate([first, second], axis=1)
    plain = both[0:8] + both[8:16]
    upper = both[16:24] + both[24:32]
    moved = pltpu.roll(upper, 1, 0)
    low_id = lax.broadcasted_iota(jnp.int32, (LOW, LANES), 0)
    moved = jnp.where(low_id == 0, pltpu.roll(moved, 1, 1), moved)
    return plain - upper + moved


def rows_kernel(
    theta_hbm,
    speed_hbm,
    tier,
    zonal_hbm,
    plan_hbm,
    energy_hbm,
    depth_hbm,
    label_hbm,
    parcel,
    last,
    south,
    theta,
    speed,
    zonal,
    plan,
    energy,
    depth,
    label,
    even,
    odd,
    field_sems,
    plane_sems,
):
    levels, parallels, width = theta.shape
    blocks = parallels // ROWS
    chunks = parallels // CHUNK

    def field_copy(which, c):
        source, target = ((theta_hbm, theta), (speed_hbm, speed))[which]
        rows = pl.ds(c * CHUNK, CHUNK)
        return pltpu.make_async_copy(
            source.at[:, rows, :], target.at[:, rows, :], field_sems.at[which, c]
        )

    planes = [
        pltpu.make_async_copy(s, t, plane_sems.at[n])
        for n, (s, t) in enumerate(
            (
                (depth_hbm, depth),
                (zonal_hbm, zonal),
                (label_hbm, label),
                (energy_hbm, energy),
                (plan_hbm, plan),
            )
        )
    ]
    field_copy(0, 0).start()
    for copy in planes:
        copy.start()
    field_copy(1, 0).start()
    for c in range(1, chunks):
        field_copy(0, c).start()
        field_copy(1, c).start()

    row_id = lax.broadcasted_iota(jnp.int32, (ROWS, width), 0)
    last_row = row_id == ROWS - 1
    lane = lax.broadcasted_iota(jnp.int32, (ROWS, LANES), 1)

    def northern(own, beyond):
        return jnp.where(last_row, jnp.broadcast_to(beyond, own.shape), pltpu.roll(own, ROWS - 1, 0))

    class Block:
        def __init__(self, block, parts):
            self.block, self.parts = block, parts
            self.rows = pl.ds(pl.multiple_of(block * ROWS, ROWS), ROWS)
            ahead = jnp.minimum(block + 1, blocks - 1) * ROWS
            self.beyond = pl.ds(pl.multiple_of(ahead, ROWS), ROWS)
            own_depth = depth[self.rows, :].astype(jnp.float32)
            next_depth = depth[self.beyond, :][0:1].astype(jnp.float32)
            next_depth = jnp.where(block == blocks - 1, 0.0, next_depth)
            self.face_depth = jnp.minimum(own_depth, northern(own_depth, next_depth))
            basin = label[self.rows, :]
            self.basin_base = basin.astype(jnp.float32) * float(HIGH)
            self.in_basin = [basin == b for b in range(OCEAN_REGIONS)]
            self.span = zonal[self.rows, :]
            self.flux = energy[self.rows, :] * plan[self.rows, :]
            self.terms = jnp.zeros((ROWS, LANES), jnp.float32)
            self.running = [jnp.zeros((ROWS, 1), jnp.float32) for _ in range(OCEAN_REGIONS)]
            self.mean_sum = jnp.zeros((ROWS, width), jnp.float32)
            self.wet_sum = jnp.zeros((ROWS, width), jnp.float32)
            self.heat_sum = jnp.zeros((ROWS, width), jnp.float32)

        def level(self, k):
            own = theta[k, self.rows, :]
            face = 0.5 * (own + northern(own, theta[k, self.beyond, :][0:1]))
            volume = jnp.where(self.face_depth > float(k), tier[k] * self.span, 0.0)
            transport = volume * speed[k, self.rows, :]
            for q, value in enumerate(interpolation(face, transport, self.basin_base)):
                self.parts[q, k] = value
            self.mean_sum += volume * face
            self.wet_sum += volume
            self.heat_sum += transport * face
            for b in range(OCEAN_REGIONS):
                self.running[b] += over_longitude(jnp.where(self.in_basin[b], transport, 0.0))
                self.terms = jnp.where(lane == b * levels + k, self.running[b], self.terms)

        def close(self):
            terms = self.terms
            for b in range(OCEAN_REGIONS):
                here = self.in_basin[b]
                heat = over_longitude(jnp.where(here, self.heat_sum, 0.0))
                terms = jnp.where(lane == HEAT + b, heat, terms)
                flux = over_longitude(jnp.where(here, self.flux, 0.0))
                terms = jnp.where(lane == FLUX + b, flux, terms)
            terms = jnp.where(lane == MEAN, over_longitude(self.mean_sum), terms)
            terms = jnp.where(lane == WET, over_longitude(self.wet_sum), terms)
            parcel[2 * self.block, TERMS : TERMS + 8, :] = terms
            parcel[2 * self.block + 1, TERMS : TERMS + 8, :] = pltpu.roll(terms, 4, 0)

    products = Products(width)

    def rows_of(parts, block, fill):
        sums = []
        for r in range(ROWS):
            spread = lambda q, k, count: jnp.broadcast_to(
                parts[q, k, r : r + 1, :], (count, width)
            )
            sums.append(products.row(spread, levels))
            for k in range(r * levels // ROWS, (r + 1) * levels // ROWS):
                fill.level(k)
        for pair in range(ROWS // 2):
            parcel[2 * block + pair // 2, 8 * (pair % 2) : 8 * (pair % 2) + 8, :] = class_tile(
                sums[2 * pair], sums[2 * pair + 1]
            )
        fill.close()

    for copy in planes:
        copy.wait()
    field_copy(0, 0).wait()
    field_copy(1, 0).wait()
    opening = Block(jnp.int32(0), even)
    for k in range(levels):
        opening.level(k)
    opening.close()

    def two_blocks(i, carry):
        @pl.when(i < chunks - 1)
        def _():
            field_copy(0, i + 1).wait()
            field_copy(1, i + 1).wait()

        rows_of(even, 2 * i, Block(2 * i + 1, odd))
        rows_of(odd, 2 * i + 1, Block(jnp.minimum(2 * i + 2, blocks - 1), even))
        return carry

    lax.fori_loop(0, chunks, two_blocks, 0)

    final = parallels - 1
    half = width // 2
    span = zonal[final : final + 1, :]
    for k in range(levels):
        last[LAST_THETA + k : LAST_THETA + k + 1, :] = theta[k, final : final + 1, :]
        last[LAST_VOLUME + k : LAST_VOLUME + k + 1, :] = tier[k] * span
        last[LAST_SPEED + k : LAST_SPEED + k + 1, :] = speed[k, final : final + 1, :]
    for k in range(levels):
        south[k : k + 1, :] = theta[k, 0:1, :]
    south[levels : levels + 1, :] = depth[0:1, :].astype(jnp.float32)
    south[levels + 1 :, :] = jnp.zeros((EDGE - levels - 1, width), jnp.float32)
    marks = (depth[final : final + 1, :] + 32 * label[final : final + 1, :]).astype(jnp.float32)
    last[LAST_MARKS : LAST_MARKS + 1, :] = marks
    last[LAST_MARKS + 1 :, :] = jnp.zeros((LAST_ROWS - LAST_MARKS - 1, width), jnp.float32)
    totals = jnp.zeros((ROWS, LANES), jnp.float32)
    for d in range(0, 2 * blocks, 2):
        totals = totals + parcel[d, TERMS : TERMS + 8, :]
    totals = jnp.sum(totals, axis=0, keepdims=True)
    for d in range(2 * blocks):
        parcel[d, TOTALS : TOTALS + 1, :] = totals
        parcel[d, TOTALS + 1 : LEVEL, :] = jnp.zeros((LEVEL - TOTALS - 1, LANES), jnp.float32)
        for n, q in enumerate((LAST_THETA + d, LAST_VOLUME + d, LAST_SPEED + d, LAST_MARKS)):
            row = last[q : q + 1, :]
            parcel[d, LEVEL + 2 * n : LEVEL + 2 * n + 1, :] = row[:, :half]
            parcel[d, LEVEL + 2 * n + 1 : LEVEL + 2 * n + 2, :] = row[:, half:]


def last_kernel(lon_size, lat_size, seam, parcels, last, halo, share, parts):
    levels = EDGE - 8
    width = last.shape[1]
    devices = parcels.shape[0]
    lon_index = lax.axis_index("lon")
    at_fold = lax.axis_index("lat") == lat_size - 1
    start = seam[0] + lon_index * width + (lon_size * width - (width - 1))
    first, offset = start // width, start % width
    total = parcels[0, 0:LEVEL, :]
    for d in range(1, devices):
        total = total + parcels[d, 0:LEVEL, :]

    def whole_row(n):
        half = lambda h: jnp.concatenate(
            [parcels[d, LEVEL + 2 * n + h : LEVEL + 2 * n + h + 1, :] for d in range(devices)], axis=0
        )
        return jnp.concatenate([half(0), half(1)], axis=1)

    def mirrored(n):
        tiles = []
        for step in range(2):
            for h in range(2):
                at = LEVEL + 2 * n + h
                tiles.append(
                    jnp.concatenate(
                        [
                            parcels[(first + (step - d)) & (devices - 1), at : at + 1, :]
                            for d in range(devices)
                        ],
                        axis=0,
                    )
                )
        return jnp.concatenate(tiles, axis=1)

    high, rest = split_in_two(mirrored(0))
    middle, lowest = split_in_two(rest)
    blocks_marks = mirrored(3)
    blocks_depth = blocks_marks - BASIN_UNIT * jnp.floor(blocks_marks * (1.0 / BASIN_UNIT))
    source = lax.broadcasted_iota(jnp.int32, (2 * width, width), 0)
    target = lax.broadcasted_iota(jnp.int32, (2 * width, width), 1)
    mirror = jnp.where(source + target == offset + (width - 1), 1.0, 0.0).astype(jnp.bfloat16)
    pieces = jnp.dot(
        jnp.concatenate([high, middle, lowest, blocks_depth], axis=0).astype(jnp.bfloat16),
        mirror,
        preferred_element_type=jnp.float32,
    )
    folded = pieces[0:16] + pieces[16:32] + pieces[32:48]

    spread_out = lambda row: jnp.broadcast_to(row, (levels, width))
    theta = jnp.where(at_fold, whole_row(0), last[LAST_THETA : LAST_THETA + levels, :])
    full_volume = jnp.where(at_fold, whole_row(1), last[LAST_VOLUME : LAST_VOLUME + levels, :])
    speed = jnp.where(at_fold, whole_row(2), last[LAST_SPEED : LAST_SPEED + levels, :])
    marks = jnp.where(at_fold, whole_row(3), spread_out(last[LAST_MARKS : LAST_MARKS + 1, :]))
    north = jnp.where(at_fold, folded, halo[0:levels, :])
    north_depth = jnp.where(at_fold, pieces[48:64], spread_out(halo[levels : levels + 1, :]))
    basin = jnp.floor(marks * (1.0 / BASIN_UNIT))
    face = 0.5 * (theta + north)
    face_depth = jnp.minimum(marks - BASIN_UNIT * basin, north_depth)
    row_id = lax.broadcasted_iota(jnp.int32, (levels, width), 0)
    level_id = jnp.where(at_fold, lon_index, row_id).astype(jnp.float32)
    volume = jnp.where(level_id < face_depth, full_volume, 0.0)
    transport = volume * speed
    for q, value in enumerate(interpolation(face, transport, basin * float(HIGH))):
        parts[q] = value
    sums = Products(width).row(
        lambda q, k, count: jnp.broadcast_to(parts[q, k : k + 1, :], (count, width)), levels
    )
    last_class = class_tile(sums, jnp.zeros_like(sums))

    lane = lax.broadcasted_iota(jnp.int32, (levels, LANES), 1)
    own_level = lax.broadcasted_iota(jnp.int32, (levels, LANES), 0)
    below = jnp.where(at_fold, lon_index, own_level) <= lane % levels
    heat = transport * face
    everything = lambda x: over_longitude(jnp.sum(x, axis=0, keepdims=True))
    running = jnp.zeros((levels, LANES), jnp.float32)
    lane1 = lane[0:1]
    terms = jnp.zeros((1, LANES), jnp.float32)
    for b in range(OCEAN_REGIONS):
        here = basin == float(b)
        level_sum = over_longitude(jnp.where(here, transport, 0.0))
        running = jnp.where((lane // levels == b) & below, level_sum, running)
        terms = jnp.where(lane1 == HEAT + b, everything(jnp.where(here, heat, 0.0)), terms)
    terms = jnp.where(lane1 == MEAN, everything(volume * face), terms)
    terms = jnp.where(lane1 == WET, everything(volume), terms)
    terms = terms + jnp.sum(running, axis=0, keepdims=True)

    place_id = lax.broadcasted_iota(jnp.int32, (EDGE, LANES), 0)
    lane24 = lax.broadcasted_iota(jnp.int32, (EDGE, LANES), 1)
    wanted = jnp.where(
        place_id < 16, (place_id & 1) * OCEAN_REGIONS + (place_id >> 2), place_id - 16
    )
    of_place = wanted == (lane24 >> 4)
    from_pair = jnp.where(place_id < 16, (place_id >> 1) & 1, 2)
    tiles = (total[0:8], total[8:16], last_class)
    wide = []
    for low in range(LOW):
        row = jnp.zeros((EDGE, LANES), jnp.float32)
        for n, tile in enumerate(tiles):
            row = jnp.where(
                of_place & (from_pair == n),
                jnp.broadcast_to(tile[low : low + 1], (EDGE, LANES)),
                row,
            )
        wide.append(row)
    wide_high, wide_low = split_in_two(jnp.concatenate(wide, axis=1))
    from_id = lax.broadcasted_iota(jnp.int32, (LANES, LANES), 0)
    to_id = lax.broadcasted_iota(jnp.int32, (LANES, LANES), 1)
    goal = (from_id & (HIGH - 1)) * LOW
    placing = jnp.concatenate(
        [jnp.where(to_id == goal + low, 1.0, 0.0) for low in range(LOW)], axis=0
    ).astype(jnp.bfloat16)
    placed = jnp.dot(
        jnp.concatenate([wide_high, wide_low], axis=0).astype(jnp.bfloat16),
        placing,
        preferred_element_type=jnp.float32,
    )
    placed = placed[0:EDGE] + placed[EDGE : 2 * EDGE]
    share[0:16, :] = placed[0:16]
    share[TERMS : TERMS + 4, :] = total[TERMS : TERMS + 4]
    share[LAST : LAST + 4, :] = placed[16:20]
    share[LAST_TERMS : LAST_TERMS + 1, :] = terms
    share[LAST_TERMS + 1 :, :] = jnp.zeros((SHARE - LAST_TERMS - 1, LANES), jnp.float32)


def finish_kernel(unit_scale, implied_scale, shares, class_out, stream, heat, implied):
    devices = shares.shape[0]
    rows = 4 * devices
    levels = stream.shape[1]
    mine = shares[0, LAST:SHARE, :]
    for d in range(1, devices):
        mine = mine + shares[d, LAST:SHARE, :]
    for b in range(OCEAN_REGIONS):
        for d in range(devices):
            class_out[b, 4 * d : 4 * d + 4, :] = unit_scale * shares[d, 4 * b : 4 * b + 4, :]
        class_out[b, rows - 1 : rows, :] += unit_scale * mine[b : b + 1]
    terms = jnp.concatenate([shares[d, TERMS : TERMS + 4, :] for d in range(devices)], axis=0)
    row_id = lax.broadcasted_iota(jnp.int32, terms.shape, 0)
    own_terms = mine[LAST_TERMS - LAST : LAST_TERMS - LAST + 1]
    terms = terms + jnp.where(row_id == rows - 1, jnp.broadcast_to(own_terms, terms.shape), 0.0)
    turned = jnp.transpose(
        jnp.concatenate([terms, jnp.zeros((LANES - rows, LANES), jnp.float32)], axis=0)
    )
    for b in range(OCEAN_REGIONS):
        stream[b] = unit_scale * turned[b * levels : (b + 1) * levels, :rows]
    lane = lax.broadcasted_iota(jnp.int32, (1, LANES), 1)
    row_mean = turned[MEAN : MEAN + 1] / jnp.where(lane < rows, turned[WET : WET + 1], 1.0)
    offsets = jnp.zeros((1, LANES), jnp.float32)
    for d in range(devices):
        offsets += shares[d, SHARE - 1 : SHARE, :]
    for b in range(OCEAN_REGIONS):
        total = turned[(b + 1) * levels - 1 : (b + 1) * levels]
        out = unit_scale / 16.0 * (turned[HEAT + b : HEAT + b + 1] - total * row_mean)
        heat[b : b + 1, :] = out[:, :rows]
        flux = turned[FLUX + b : FLUX + b + 1]
        offset = over_longitude(jnp.where(lane == FLUX + b, offsets, 0.0))
        shift = 1
        while shift < rows:
            flux = flux + jnp.where(lane >= shift, pltpu.roll(flux, shift, 1), 0.0)
            shift *= 2
        implied[b : b + 1, :] = (implied_scale * (flux + offset))[:, :rows]


def exchanged(pieces, axis):
    return lax.all_to_all(pieces, axis, split_axis=0, concat_axis=0, tiled=True)


def body(
    meridional_speed,
    theta_field,
    tier_vertical_span,
    grid_zonal_span,
    grid_plan_extent,
    ocean_energy_input,
    ocean_tier_tally,
    grid_region_label,
    seam_matching_meridian,
):
    levels, parallels, width = theta_field.shape
    lon_size = lax.axis_size("lon")
    lat_size = lax.axis_size("lat")
    width_total = width * lon_size
    unit_scale = math.sqrt(THERMAL_BINS / (width_total * levels))
    implied_scale = 2.0 / math.sqrt(width_total * parallels * lat_size)
    blocks = parallels // ROWS
    chunks = parallels // CHUNK

    in_smem = pl.BlockSpec(memory_space=pltpu.SMEM)
    in_vmem = pl.BlockSpec(memory_space=pltpu.VMEM)
    anywhere = pl.BlockSpec(memory_space=pl.ANY)
    plane_f32 = pltpu.VMEM((parallels, width), jnp.float32)
    plane_i32 = pltpu.VMEM((parallels, width), jnp.int32)
    field = pltpu.VMEM((levels, parallels, width), jnp.float32)
    parts = pltpu.VMEM((6, levels, ROWS, width), jnp.float32)
    parcels, last, southernmost = pl.pallas_call(
        rows_kernel,
        in_specs=[anywhere, anywhere, in_smem] + [anywhere] * 5,
        out_specs=(in_vmem,) * 3,
        out_shape=(
            jax.ShapeDtypeStruct((2 * blocks, PARCEL, LANES), jnp.float32),
            jax.ShapeDtypeStruct((LAST_ROWS, width), jnp.float32),
            jax.ShapeDtypeStruct((EDGE, width), jnp.float32),
        ),
        scratch_shapes=[
            field,
            field,
            plane_f32,
            plane_f32,
            plane_f32,
            plane_i32,
            plane_i32,
            parts,
            parts,
            pltpu.SemaphoreType.DMA((2, chunks)),
            pltpu.SemaphoreType.DMA((5,)),
        ],
        cost_estimate=pl.CostEstimate(
            flops=8_000_000_000, bytes_accessed=4_000_000, transcendentals=0
        ),
        name="rows",
    )(
        theta_field,
        meridional_speed,
        tier_vertical_span,
        grid_zonal_span,
        grid_plan_extent,
        ocean_energy_input,
        ocean_tier_tally,
        grid_region_label,
    )
    received = exchanged(parcels, "lon")
    halo = lax.ppermute(southernmost, "lat", [(i + 1, i) for i in range(lat_size - 1)])
    row_flux = jnp.sum(received[:, TOTALS, :], axis=0)[None]
    northward = [
        (r * lat_size + s, r * lat_size + s + r)
        for r in range(1, lon_size)
        for s in range(lat_size - r)
    ]
    of_block = lax.ppermute(row_flux, ("lon", "lat"), northward)
    share = pl.pallas_call(
        functools.partial(last_kernel, lon_size, lat_size),
        in_specs=[in_smem, in_vmem, in_vmem, in_vmem],
        out_specs=in_vmem,
        out_shape=jax.ShapeDtypeStruct((SHARE, LANES), jnp.float32),
        scratch_shapes=[
            pltpu.VMEM((6, levels, width), jnp.float32),
        ],
        compiler_params=pltpu.CompilerParams(vmem_limit_bytes=SMALL_KERNEL),
        cost_estimate=pl.CostEstimate(
            flops=1_000_000_000, bytes_accessed=600_000, transcendentals=0
        ),
        name="last_row",
    )(seam_matching_meridian, received, last, halo)
    row_id = lax.broadcasted_iota(jnp.int32, share.shape, 0)
    share = jnp.where(row_id == SHARE - 1, of_block, share)
    shares = exchanged(jnp.broadcast_to(share, (lon_size, SHARE, LANES)), "lon")
    class_out, stream, heat, implied = pl.pallas_call(
        functools.partial(finish_kernel, unit_scale, implied_scale),
        in_specs=[in_vmem],
        out_specs=(in_vmem,) * 4,
        out_shape=(
            jax.ShapeDtypeStruct((OCEAN_REGIONS, parallels, THERMAL_BINS), jnp.float32),
            jax.ShapeDtypeStruct((OCEAN_REGIONS, levels, parallels), jnp.float32),
            jax.ShapeDtypeStruct((OCEAN_REGIONS, parallels), jnp.float32),
            jax.ShapeDtypeStruct((OCEAN_REGIONS, parallels), jnp.float32),
        ),
        compiler_params=pltpu.CompilerParams(vmem_limit_bytes=SMALL_KERNEL),
        name="finish",
    )(shares)
    return class_out, jnp.transpose(stream, (0, 2, 1)), heat, implied


def solution(mesh):
    in_specs = (
        P(None, "lat", "lon"),
        P(None, "lat", "lon"),
        P(),
        P("lat", "lon"),
        P("lat", "lon"),
        P("lat", "lon"),
        P("lat", "lon"),
        P("lat", "lon"),
        P("lon"),
    )
    out_specs = (P(None, "lat", None), P(None, "lat", None), P(None, "lat"), P(None, "lat"))
    return jax.shard_map(body, mesh=mesh, in_specs=in_specs, out_specs=out_specs, check_vma=False)
```

```python
import functools
import math

import jax
import jax.numpy as jnp
from jax import lax
from jax.experimental import pallas as pl
from jax.experimental.pallas import tpu as pltpu
from jax.sharding import PartitionSpec as P

THERMAL_BINS = 128
OCEAN_REGIONS = 4
THERMAL_FLOOR = -2.0
THERMAL_RANGE = 32.0

ROWS = 8
CHUNK = 16
LOW = 8
HIGH = THERMAL_BINS // LOW
GROUPS = OCEAN_REGIONS * HIGH
LANES = 128
EDGE = 24
TERMS, TOTALS, LEVEL, PARCEL = 16, 20, 22, 32
LAST, SHARE = 20, 24
EXTRA = 96
SMALL_KERNEL = 8 * 1024 * 1024
LAST_THETA, LAST_VOLUME, LAST_SPEED, LAST_DEPTH, LAST_BASIN, LAST_ROWS = 0, 16, 32, 48, 49, 56
HEAT, FLUX, MEAN, WET = 64, 68, 76, 77


def split_in_two(x):
    high = x.astype(jnp.bfloat16).astype(jnp.float32)
    return high, x - high


def over_longitude(x):
    return jnp.sum(x, axis=1, keepdims=True)


def interpolation(face, transport, basin_base):
    per_bin = THERMAL_BINS / THERMAL_RANGE
    position = jnp.clip((face - THERMAL_FLOOR) * per_bin, 0.0, THERMAL_BINS - 1.0)
    low_bin = jnp.minimum(jnp.floor(position), THERMAL_BINS - 2.0)
    digit = jnp.floor(low_bin * (1.0 / LOW))
    weighted = transport * (position - low_bin)
    return (
        basin_base + digit,
        low_bin - LOW * digit,
        *split_in_two(transport),
        *split_in_two(weighted),
    )


class Products:
    def __init__(self, width):
        packed_id = lax.broadcasted_iota(jnp.int32, (16, width), 0)
        as_packed = lambda x: x.astype(jnp.float32).astype(jnp.bfloat16)
        self.group_ids = [as_packed(packed_id + 16 * t) for t in range(GROUPS // 16)]
        self.low_ids = as_packed(packed_id & (LOW - 1))
        self.one = jnp.ones((16, width), jnp.bfloat16)
        self.none = jnp.zeros((16, width), jnp.bfloat16)
        self.width = width

    def row(self, spread, levels):
        values, groups = [], []
        for k in range(levels):
            group = spread(0, k, 16).astype(jnp.bfloat16)
            groups.append(
                jnp.concatenate(
                    [jnp.where(group == g, self.one, self.none) for g in self.group_ids], axis=0
                )
            )
            at_low = spread(1, k, 16).astype(jnp.bfloat16) == self.low_ids
            values.append(
                jnp.concatenate(
                    [
                        jnp.where(
                            at_low,
                            jnp.concatenate([spread(q, k, 8), spread(q + 1, k, 8)], axis=0).astype(
                                jnp.bfloat16
                            ),
                            self.none,
                        )
                        for q in (2, 4)
                    ],
                    axis=0,
                )
            )
        return values, groups

    def alone(self, spread, levels):
        values, groups = self.row(spread, levels)
        return lax.dot_general(
            jnp.concatenate(values, axis=1),
            jnp.concatenate(groups, axis=1),
            (((1,), (1,)), ((), ())),
            preferred_element_type=jnp.float32,
        )

    def pair(self, spreads, levels):
        rows = [self.row(spread, levels) for spread in spreads]
        left = [g if n % 2 else v for n, (v, g) in enumerate(rows)]
        right = [v if n % 2 else g for n, (v, g) in enumerate(rows)]
        join = lambda sides: jnp.concatenate(
            [jnp.concatenate([side[k] for side in sides], axis=0) for k in range(levels)], axis=1
        )
        out = lax.dot_general(
            join(left), join(right), (((1,), (1,)), ((), ())), preferred_element_type=jnp.float32
        )
        sums = []
        for n in range(0, len(rows), 2):
            o = 96 * (n // 2)
            sums += [out[o : o + 32, o : o + 64], jnp.transpose(out[o + 32 : o + 96, o + 64 : o + 96])]
        return sums


def class_tile(first, second):
    both = jnp.concatenate([first, second], axis=1)
    plain = both[0:8] + both[8:16]
    upper = both[16:24] + both[24:32]
    moved = pltpu.roll(upper, 1, 0)
    low_id = lax.broadcasted_iota(jnp.int32, (LOW, LANES), 0)
    moved = jnp.where(low_id == 0, pltpu.roll(moved, 1, 1), moved)
    return plain - upper + moved


def rows_kernel(
    theta_hbm,
    speed_hbm,
    tier,
    zonal_hbm,
    plan_hbm,
    energy_hbm,
    depth_hbm,
    label_hbm,
    parcel,
    last,
    south,
    theta,
    speed,
    zonal,
    plan,
    energy,
    depth,
    label,
    even,
    odd,
    field_sems,
    plane_sems,
):
    levels, parallels, width = theta.shape
    blocks = parallels // ROWS
    chunks = parallels // CHUNK

    def field_copy(which, c):
        source, target = ((theta_hbm, theta), (speed_hbm, speed))[which]
        rows = pl.ds(c * CHUNK, CHUNK)
        return pltpu.make_async_copy(
            source.at[:, rows, :], target.at[:, rows, :], field_sems.at[which, c]
        )

    planes = [
        pltpu.make_async_copy(s, t, plane_sems.at[n])
        for n, (s, t) in enumerate(
            (
                (depth_hbm, depth),
                (zonal_hbm, zonal),
                (label_hbm, label),
                (energy_hbm, energy),
                (plan_hbm, plan),
            )
        )
    ]
    field_copy(0, 0).start()
    for copy in planes:
        copy.start()
    field_copy(1, 0).start()
    for c in range(1, chunks):
        field_copy(0, c).start()
        field_copy(1, c).start()

    row_id = lax.broadcasted_iota(jnp.int32, (ROWS, width), 0)
    last_row = row_id == ROWS - 1
    lane = lax.broadcasted_iota(jnp.int32, (ROWS, LANES), 1)

    def northern(own, beyond):
        return jnp.where(last_row, jnp.broadcast_to(beyond, own.shape), pltpu.roll(own, ROWS - 1, 0))

    class Block:
        def __init__(self, block, parts):
            self.block, self.parts = block, parts
            self.rows = pl.ds(pl.multiple_of(block * ROWS, ROWS), ROWS)
            ahead = jnp.minimum(block + 1, blocks - 1) * ROWS
            self.beyond = pl.ds(pl.multiple_of(ahead, ROWS), ROWS)
            own_depth = depth[self.rows, :].astype(jnp.float32)
            next_depth = depth[self.beyond, :][0:1].astype(jnp.float32)
            next_depth = jnp.where(block == blocks - 1, 0.0, next_depth)
            self.face_depth = jnp.minimum(own_depth, northern(own_depth, next_depth))
            basin = label[self.rows, :]
            self.basin_base = basin.astype(jnp.float32) * float(HIGH)
            self.in_basin = [basin == b for b in range(OCEAN_REGIONS)]
            self.span = zonal[self.rows, :]
            self.flux = energy[self.rows, :] * plan[self.rows, :]
            self.terms = jnp.zeros((ROWS, LANES), jnp.float32)
            self.running = [jnp.zeros((ROWS, 1), jnp.float32) for _ in range(OCEAN_REGIONS)]
            self.mean_sum = jnp.zeros((ROWS, width), jnp.float32)
            self.wet_sum = jnp.zeros((ROWS, width), jnp.float32)
            self.heat_sum = jnp.zeros((ROWS, width), jnp.float32)

        def level(self, k):
            own = theta[k, self.rows, :]
            face = 0.5 * (own + northern(own, theta[k, self.beyond, :][0:1]))
            volume = jnp.where(self.face_depth > float(k), tier[k] * self.span, 0.0)
            transport = volume * speed[k, self.rows, :]
            for q, value in enumerate(interpolation(face, transport, self.basin_base)):
                self.parts[q, k] = value
            self.mean_sum += volume * face
            self.wet_sum += volume
            self.heat_sum += transport * face
            for b in range(OCEAN_REGIONS):
                self.running[b] += over_longitude(jnp.where(self.in_basin[b], transport, 0.0))
                self.terms = jnp.where(lane == b * levels + k, self.running[b], self.terms)

        def close(self):
            terms = self.terms
            for b in range(OCEAN_REGIONS):
                here = self.in_basin[b]
                heat = over_longitude(jnp.where(here, self.heat_sum, 0.0))
                terms = jnp.where(lane == HEAT + b, heat, terms)
                flux = over_longitude(jnp.where(here, self.flux, 0.0))
                terms = jnp.where(lane == FLUX + b, flux, terms)
            terms = jnp.where(lane == MEAN, over_longitude(self.mean_sum), terms)
            terms = jnp.where(lane == WET, over_longitude(self.wet_sum), terms)
            parcel[2 * self.block, TERMS : TERMS + 8, :] = terms
            parcel[2 * self.block + 1, TERMS : TERMS + 8, :] = pltpu.roll(terms, 4, 0)

    products = Products(width)

    def rows_of(parts, block, fill):
        sums = []
        for start in range(0, ROWS, 2):
            spreads = [
                lambda q, k, count, r=r: jnp.broadcast_to(parts[q, k, r : r + 1, :], (count, width))
                for r in range(start, start + 2)
            ]
            sums += products.pair(spreads, levels)
            for k in range(start * levels // ROWS, (start + 2) * levels // ROWS):
                fill.level(k)
        for pair in range(ROWS // 2):
            parcel[2 * block + pair // 2, 8 * (pair % 2) : 8 * (pair % 2) + 8, :] = class_tile(
                sums[2 * pair], sums[2 * pair + 1]
            )
        fill.close()

    for copy in planes:
        copy.wait()
    field_copy(0, 0).wait()
    field_copy(1, 0).wait()
    opening = Block(jnp.int32(0), even)
    for k in range(levels):
        opening.level(k)
    opening.close()

    def two_blocks(i, carry):
        @pl.when(i < chunks - 1)
        def _():
            field_copy(0, i + 1).wait()
            field_copy(1, i + 1).wait()

        rows_of(even, 2 * i, Block(2 * i + 1, odd))
        rows_of(odd, 2 * i + 1, Block(jnp.minimum(2 * i + 2, blocks - 1), even))
        return carry

    lax.fori_loop(0, chunks, two_blocks, 0)

    final = parallels - 1
    half = width // 2
    span = zonal[final : final + 1, :]
    for k in range(levels):
        last[LAST_THETA + k : LAST_THETA + k + 1, :] = theta[k, final : final + 1, :]
        last[LAST_VOLUME + k : LAST_VOLUME + k + 1, :] = tier[k] * span
        last[LAST_SPEED + k : LAST_SPEED + k + 1, :] = speed[k, final : final + 1, :]
    for k in range(levels):
        south[k : k + 1, :] = theta[k, 0:1, :]
    south[levels : levels + 1, :] = depth[0:1, :].astype(jnp.float32)
    south[levels + 1 :, :] = jnp.zeros((EDGE - levels - 1, width), jnp.float32)
    last[LAST_DEPTH : LAST_DEPTH + 1, :] = depth[final : final + 1, :].astype(jnp.float32)
    last[LAST_BASIN : LAST_BASIN + 1, :] = label[final : final + 1, :].astype(jnp.float32)
    last[LAST_BASIN + 1 :, :] = jnp.zeros((LAST_ROWS - LAST_BASIN - 1, width), jnp.float32)
    totals = jnp.zeros((ROWS, LANES), jnp.float32)
    for d in range(0, 2 * blocks, 2):
        totals = totals + parcel[d, TERMS : TERMS + 8, :]
    totals = pltpu.roll(jnp.sum(totals, axis=0, keepdims=True), LANES // 4, 1)
    for d in range(2 * blocks):
        parcel[d, TOTALS : TOTALS + 1, :] = totals
        parcel[d, TOTALS + 1 : LEVEL, :] = jnp.zeros((LEVEL - TOTALS - 1, LANES), jnp.float32)
        for n, q in enumerate(
            (LAST_THETA + d, LAST_VOLUME + d, LAST_SPEED + d, LAST_DEPTH, LAST_BASIN)
        ):
            row = last[q : q + 1, :]
            parcel[d, LEVEL + 2 * n : LEVEL + 2 * n + 1, :] = row[:, :half]
            parcel[d, LEVEL + 2 * n + 1 : LEVEL + 2 * n + 2, :] = row[:, half:]


def last_kernel(lon_size, lat_size, seam, parcels, last, halo, share, parts):
    levels = EDGE - 8
    width = last.shape[1]
    devices = parcels.shape[0]
    lon_index = lax.axis_index("lon")
    at_fold = lax.axis_index("lat") == lat_size - 1
    start = seam[0] + lon_index * width + (lon_size * width - (width - 1))
    first, offset = start // width, start % width
    total = parcels[0, 0:LEVEL, :]
    for d in range(1, devices):
        total = total + parcels[d, 0:LEVEL, :]

    def whole_row(n):
        half = lambda h: jnp.concatenate(
            [parcels[d, LEVEL + 2 * n + h : LEVEL + 2 * n + h + 1, :] for d in range(devices)], axis=0
        )
        return jnp.concatenate([half(0), half(1)], axis=1)

    def mirrored(n):
        tiles = []
        for step in range(2):
            for h in range(2):
                at = LEVEL + 2 * n + h
                tiles.append(
                    jnp.concatenate(
                        [
                            parcels[(first + (step - d)) & (devices - 1), at : at + 1, :]
                            for d in range(devices)
                        ],
                        axis=0,
                    )
                )
        return jnp.concatenate(tiles, axis=1)

    high, rest = split_in_two(mirrored(0))
    middle, lowest = split_in_two(rest)
    source = lax.broadcasted_iota(jnp.int32, (2 * width, width), 0)
    target = lax.broadcasted_iota(jnp.int32, (2 * width, width), 1)
    mirror = jnp.where(source + target == offset + (width - 1), 1.0, 0.0).astype(jnp.bfloat16)
    pieces = jnp.dot(
        jnp.concatenate([high, middle, lowest, mirrored(3)], axis=0).astype(jnp.bfloat16),
        mirror,
        preferred_element_type=jnp.float32,
    )
    folded = pieces[0:16] + pieces[16:32] + pieces[32:48]

    spread_out = lambda row: jnp.broadcast_to(row, (levels, width))
    theta = jnp.where(at_fold, whole_row(0), last[LAST_THETA : LAST_THETA + levels, :])
    full_volume = jnp.where(at_fold, whole_row(1), last[LAST_VOLUME : LAST_VOLUME + levels, :])
    speed = jnp.where(at_fold, whole_row(2), last[LAST_SPEED : LAST_SPEED + levels, :])
    depth = jnp.where(at_fold, whole_row(3), spread_out(last[LAST_DEPTH : LAST_DEPTH + 1, :]))
    basin = jnp.where(at_fold, whole_row(4), spread_out(last[LAST_BASIN : LAST_BASIN + 1, :]))
    north = jnp.where(at_fold, folded, halo[0:levels, :])
    north_depth = jnp.where(at_fold, pieces[48:64], spread_out(halo[levels : levels + 1, :]))
    face = 0.5 * (theta + north)
    face_depth = jnp.minimum(depth, north_depth)
    row_id = lax.broadcasted_iota(jnp.int32, (levels, width), 0)
    level_id = jnp.where(at_fold, lon_index, row_id).astype(jnp.float32)
    volume = jnp.where(level_id < face_depth, full_volume, 0.0)
    transport = volume * speed
    for q, value in enumerate(interpolation(face, transport, basin * float(HIGH))):
        parts[q] = value
    sums = Products(width).alone(
        lambda q, k, count: jnp.broadcast_to(parts[q, k : k + 1, :], (count, width)), levels
    )
    last_class = class_tile(sums, jnp.zeros_like(sums))

    lane = lax.broadcasted_iota(jnp.int32, (levels, LANES), 1)
    own_level = lax.broadcasted_iota(jnp.int32, (levels, LANES), 0)
    below = jnp.where(at_fold, lon_index, own_level) <= lane % levels
    heat = transport * face
    everything = lambda x: over_longitude(jnp.sum(x, axis=0, keepdims=True))
    running = jnp.zeros((levels, LANES), jnp.float32)
    lane1 = lane[0:1]
    terms = jnp.zeros((1, LANES), jnp.float32)
    for b in range(OCEAN_REGIONS):
        here = basin == float(b)
        level_sum = over_longitude(jnp.where(here, transport, 0.0))
        running = jnp.where((lane // levels == b) & below, level_sum, running)
        terms = jnp.where(lane1 == HEAT + b, everything(jnp.where(here, heat, 0.0)), terms)
    terms = jnp.where(lane1 == MEAN, everything(volume * face), terms)
    terms = jnp.where(lane1 == WET, everything(volume), terms)
    terms = terms + jnp.sum(running, axis=0, keepdims=True)

    place_id = lax.broadcasted_iota(jnp.int32, (EDGE, LANES), 0)
    lane24 = lax.broadcasted_iota(jnp.int32, (EDGE, LANES), 1)
    wanted = jnp.where(
        place_id < 16, (place_id & 1) * OCEAN_REGIONS + (place_id >> 2), place_id - 16
    )
    of_place = wanted == (lane24 >> 4)
    from_pair = jnp.where(place_id < 16, (place_id >> 1) & 1, 2)
    tiles = (total[0:8], total[8:16], last_class)
    wide = []
    for low in range(LOW):
        row = jnp.zeros((EDGE, LANES), jnp.float32)
        for n, tile in enumerate(tiles):
            row = jnp.where(
                of_place & (from_pair == n),
                jnp.broadcast_to(tile[low : low + 1], (EDGE, LANES)),
                row,
            )
        wide.append(row)
    wide_high, wide_low = split_in_two(jnp.concatenate(wide, axis=1))
    from_id = lax.broadcasted_iota(jnp.int32, (LANES, LANES), 0)
    to_id = lax.broadcasted_iota(jnp.int32, (LANES, LANES), 1)
    goal = (from_id & (HIGH - 1)) * LOW
    placing = jnp.concatenate(
        [jnp.where(to_id == goal + low, 1.0, 0.0) for low in range(LOW)], axis=0
    ).astype(jnp.bfloat16)
    placed = jnp.dot(
        jnp.concatenate([wide_high, wide_low], axis=0).astype(jnp.bfloat16),
        placing,
        preferred_element_type=jnp.float32,
    )
    placed = placed[0:EDGE] + placed[EDGE : 2 * EDGE]
    share[0:16, :] = placed[0:16]
    for n in range(4):
        own = pltpu.roll(terms, EXTRA - n * (LANES // 4), 1)
        share[TERMS + n : TERMS + n + 1, :] = jnp.where(
            lane1 >= EXTRA, own, total[TERMS + n : TERMS + n + 1]
        )
    share[LAST : LAST + 4, :] = placed[16:20]


def finish_kernel(unit_scale, implied_scale, shares, class_out, stream, heat, implied):
    devices = shares.shape[0]
    rows = 4 * devices
    levels = stream.shape[1]
    mine = shares[0, TERMS:SHARE, :]
    for d in range(1, devices):
        mine = mine + shares[d, TERMS:SHARE, :]
    lane = lax.broadcasted_iota(jnp.int32, (1, LANES), 1)
    own_terms = jnp.zeros((1, LANES), jnp.float32)
    for n in range(3):
        quarter = pltpu.roll(mine[n : n + 1], (n + 1) * (LANES // 4), 1)
        own_terms = jnp.where(lane // (LANES // 4) == n, quarter, own_terms)
    offsets = mine[3:4]
    for b in range(OCEAN_REGIONS):
        for d in range(devices):
            class_out[b, 4 * d : 4 * d + 4, :] = unit_scale * shares[d, 4 * b : 4 * b + 4, :]
        class_out[b, rows - 1 : rows, :] += unit_scale * mine[LAST - TERMS + b : LAST - TERMS + b + 1]
    terms = jnp.concatenate([shares[d, TERMS : TERMS + 4, :] for d in range(devices)], axis=0)
    row_id = lax.broadcasted_iota(jnp.int32, terms.shape, 0)
    terms = terms + jnp.where(row_id == rows - 1, jnp.broadcast_to(own_terms, terms.shape), 0.0)
    turned = jnp.transpose(
        jnp.concatenate([terms, jnp.zeros((LANES - rows, LANES), jnp.float32)], axis=0)
    )
    for b in range(OCEAN_REGIONS):
        stream[b] = unit_scale * turned[b * levels : (b + 1) * levels, :rows]
    row_mean = turned[MEAN : MEAN + 1] / jnp.where(lane < rows, turned[WET : WET + 1], 1.0)
    for b in range(OCEAN_REGIONS):
        total = turned[(b + 1) * levels - 1 : (b + 1) * levels]
        out = unit_scale / 16.0 * (turned[HEAT + b : HEAT + b + 1] - total * row_mean)
        heat[b : b + 1, :] = out[:, :rows]
        flux = turned[FLUX + b : FLUX + b + 1]
        offset = over_longitude(jnp.where(lane == FLUX + LANES // 4 + b, offsets, 0.0))
        shift = 1
        while shift < rows:
            flux = flux + jnp.where(lane >= shift, pltpu.roll(flux, shift, 1), 0.0)
            shift *= 2
        implied[b : b + 1, :] = (implied_scale * (flux + offset))[:, :rows]


def exchanged(pieces, axis):
    return lax.all_to_all(pieces, axis, split_axis=0, concat_axis=0, tiled=True)


def body(
    meridional_speed,
    theta_field,
    tier_vertical_span,
    grid_zonal_span,
    grid_plan_extent,
    ocean_energy_input,
    ocean_tier_tally,
    grid_region_label,
    seam_matching_meridian,
):
    levels, parallels, width = theta_field.shape
    lon_size = lax.axis_size("lon")
    lat_size = lax.axis_size("lat")
    width_total = width * lon_size
    unit_scale = math.sqrt(THERMAL_BINS / (width_total * levels))
    implied_scale = 2.0 / math.sqrt(width_total * parallels * lat_size)
    blocks = parallels // ROWS
    chunks = parallels // CHUNK

    in_smem = pl.BlockSpec(memory_space=pltpu.SMEM)
    in_vmem = pl.BlockSpec(memory_space=pltpu.VMEM)
    anywhere = pl.BlockSpec(memory_space=pl.ANY)
    plane_f32 = pltpu.VMEM((parallels, width), jnp.float32)
    plane_i32 = pltpu.VMEM((parallels, width), jnp.int32)
    field = pltpu.VMEM((levels, parallels, width), jnp.float32)
    parts = pltpu.VMEM((6, levels, ROWS, width), jnp.float32)
    parcels, last, southernmost = pl.pallas_call(
        rows_kernel,
        in_specs=[anywhere, anywhere, in_smem] + [anywhere] * 5,
        out_specs=(in_vmem,) * 3,
        out_shape=(
            jax.ShapeDtypeStruct((2 * blocks, PARCEL, LANES), jnp.float32),
            jax.ShapeDtypeStruct((LAST_ROWS, width), jnp.float32),
            jax.ShapeDtypeStruct((EDGE, width), jnp.float32),
        ),
        scratch_shapes=[
            field,
            field,
            plane_f32,
            plane_f32,
            plane_f32,
            plane_i32,
            plane_i32,
            parts,
            parts,
            pltpu.SemaphoreType.DMA((2, chunks)),
            pltpu.SemaphoreType.DMA((5,)),
        ],
        cost_estimate=pl.CostEstimate(
            flops=8_000_000_000, bytes_accessed=4_000_000, transcendentals=0
        ),
        name="rows",
    )(
        theta_field,
        meridional_speed,
        tier_vertical_span,
        grid_zonal_span,
        grid_plan_extent,
        ocean_energy_input,
        ocean_tier_tally,
        grid_region_label,
    )
    received = exchanged(parcels, "lon")
    halo = lax.ppermute(southernmost, "lat", [(i + 1, i) for i in range(lat_size - 1)])
    row_flux = jnp.sum(received[:, TOTALS, :], axis=0)[None]
    northward = [
        (r * lat_size + s, r * lat_size + s + r)
        for r in range(1, lon_size)
        for s in range(lat_size - r)
    ]
    of_block = lax.ppermute(row_flux, ("lon", "lat"), northward)
    share = pl.pallas_call(
        functools.partial(last_kernel, lon_size, lat_size),
        in_specs=[in_smem, in_vmem, in_vmem, in_vmem],
        out_specs=in_vmem,
        out_shape=jax.ShapeDtypeStruct((SHARE, LANES), jnp.float32),
        scratch_shapes=[
            pltpu.VMEM((6, levels, width), jnp.float32),
        ],
        compiler_params=pltpu.CompilerParams(vmem_limit_bytes=SMALL_KERNEL),
        cost_estimate=pl.CostEstimate(
            flops=1_000_000_000, bytes_accessed=600_000, transcendentals=0
        ),
        name="last_row",
    )(seam_matching_meridian, received, last, halo)
    row_id = lax.broadcasted_iota(jnp.int32, share.shape, 0)
    lane = lax.broadcasted_iota(jnp.int32, share.shape, 1)
    share = jnp.where((row_id == TERMS + 3) & (lane >= EXTRA), of_block, share)
    shares = exchanged(jnp.broadcast_to(share, (lon_size, SHARE, LANES)), "lon")
    class_out, stream, heat, implied = pl.pallas_call(
        functools.partial(finish_kernel, unit_scale, implied_scale),
        in_specs=[in_vmem],
        out_specs=(in_vmem,) * 4,
        out_shape=(
            jax.ShapeDtypeStruct((OCEAN_REGIONS, parallels, THERMAL_BINS), jnp.float32),
            jax.ShapeDtypeStruct((OCEAN_REGIONS, levels, parallels), jnp.float32),
            jax.ShapeDtypeStruct((OCEAN_REGIONS, parallels), jnp.float32),
            jax.ShapeDtypeStruct((OCEAN_REGIONS, parallels), jnp.float32),
        ),
        compiler_params=pltpu.CompilerParams(vmem_limit_bytes=SMALL_KERNEL),
        name="finish",
    )(shares)
    return class_out, jnp.transpose(stream, (0, 2, 1)), heat, implied


def solution(mesh):
    in_specs = (
        P(None, "lat", "lon"),
        P(None, "lat", "lon"),
        P(),
        P("lat", "lon"),
        P("lat", "lon"),
        P("lat", "lon"),
        P("lat", "lon"),
        P("lat", "lon"),
        P("lon"),
    )
    out_specs = (P(None, "lat", None), P(None, "lat", None), P(None, "lat"), P(None, "lat"))
    return jax.shard_map(body, mesh=mesh, in_specs=in_specs, out_specs=out_specs, check_vma=False)
```

```python
import functools
import math

import jax
import jax.numpy as jnp
from jax import lax
from jax.experimental import pallas as pl
from jax.experimental.pallas import tpu as pltpu
from jax.sharding import PartitionSpec as P

THERMAL_BINS = 128
OCEAN_REGIONS = 4
THERMAL_FLOOR = -2.0
THERMAL_RANGE = 32.0

ROWS = 8
CHUNK = 16
LOW = 8
HIGH = THERMAL_BINS // LOW
GROUPS = OCEAN_REGIONS * HIGH
LANES = 128
EDGE = 24
TERMS, TOTALS, LEVEL, PARCEL = 16, 20, 22, 32
LAST, SHARE = 20, 24
EXTRA = 96
SMALL_KERNEL = 8 * 1024 * 1024
LAST_THETA, LAST_VOLUME, LAST_SPEED, LAST_DEPTH, LAST_BASIN, LAST_ROWS = 0, 16, 32, 48, 49, 56
HEAT, FLUX, MEAN, WET = 64, 68, 76, 77


def split_in_two(x):
    high = x.astype(jnp.bfloat16).astype(jnp.float32)
    return high, x - high


def over_longitude(x):
    return jnp.sum(x, axis=1, keepdims=True)


def interpolation(face, transport):
    per_bin = THERMAL_BINS / THERMAL_RANGE
    position = jnp.clip((face - THERMAL_FLOOR) * per_bin, 0.0, THERMAL_BINS - 1.0)
    low_bin = jnp.minimum(jnp.floor(position), THERMAL_BINS - 2.0)
    digit = jnp.floor(low_bin * (1.0 / LOW))
    weighted = transport * (position - low_bin)
    return (
        digit,
        low_bin - LOW * digit,
        *split_in_two(transport),
        *split_in_two(weighted),
    )


class Products:
    def __init__(self, width):
        packed_id = lax.broadcasted_iota(jnp.int32, (16, width), 0)
        as_packed = lambda x: x.astype(jnp.float32).astype(jnp.bfloat16)
        self.high_ids = as_packed(packed_id)
        self.low_ids = as_packed(packed_id & (LOW - 1))
        self.one = jnp.ones((16, width), jnp.bfloat16)
        self.none = jnp.zeros((16, width), jnp.bfloat16)
        self.width = width

    def indicators(self, basin):
        basin = basin.astype(jnp.bfloat16)
        return [jnp.where(basin == b, self.one, self.none) for b in range(OCEAN_REGIONS)]

    def row(self, spread, in_basin, levels):
        values, groups = [], []
        for k in range(levels):
            at_high = spread(0, k, 16).astype(jnp.bfloat16) == self.high_ids
            at_high = jnp.where(at_high, self.one, self.none)
            groups.append(jnp.concatenate([at_high * x for x in in_basin(k)], axis=0))
            at_low = spread(1, k, 16).astype(jnp.bfloat16) == self.low_ids
            values.append(
                jnp.concatenate(
                    [
                        jnp.where(
                            at_low,
                            jnp.concatenate([spread(q, k, 8), spread(q + 1, k, 8)], axis=0).astype(
                                jnp.bfloat16
                            ),
                            self.none,
                        )
                        for q in (2, 4)
                    ],
                    axis=0,
                )
            )
        return values, groups

    def alone(self, spread, in_basin, levels):
        values, groups = self.row(spread, in_basin, levels)
        return lax.dot_general(
            jnp.concatenate(values, axis=1),
            jnp.concatenate(groups, axis=1),
            (((1,), (1,)), ((), ())),
            preferred_element_type=jnp.float32,
        )

    def pair(self, spreads, basins, levels):
        rows = []
        for spread, basin in zip(spreads, basins):
            here = self.indicators(basin)
            rows.append(self.row(spread, lambda k, here=here: here, levels))
        left = [g if n % 2 else v for n, (v, g) in enumerate(rows)]
        right = [v if n % 2 else g for n, (v, g) in enumerate(rows)]
        join = lambda sides: jnp.concatenate(
            [jnp.concatenate([side[k] for side in sides], axis=0) for k in range(levels)], axis=1
        )
        out = lax.dot_general(
            join(left), join(right), (((1,), (1,)), ((), ())), preferred_element_type=jnp.float32
        )
        sums = []
        for n in range(0, len(rows), 2):
            o = 96 * (n // 2)
            sums += [out[o : o + 32, o : o + 64], jnp.transpose(out[o + 32 : o + 96, o + 64 : o + 96])]
        return sums


def class_tile(first, second):
    both = jnp.concatenate([first, second], axis=1)
    plain = both[0:8] + both[8:16]
    upper = both[16:24] + both[24:32]
    moved = pltpu.roll(upper, 1, 0)
    low_id = lax.broadcasted_iota(jnp.int32, (LOW, LANES), 0)
    moved = jnp.where(low_id == 0, pltpu.roll(moved, 1, 1), moved)
    return plain - upper + moved


def rows_kernel(
    theta_hbm,
    speed_hbm,
    tier,
    zonal_hbm,
    plan_hbm,
    energy_hbm,
    depth_hbm,
    label_hbm,
    parcel,
    last,
    south,
    theta,
    speed,
    zonal,
    plan,
    energy,
    depth,
    label,
    even,
    odd,
    even_basins,
    odd_basins,
    field_sems,
    plane_sems,
):
    levels, parallels, width = theta.shape
    blocks = parallels // ROWS
    chunks = parallels // CHUNK

    def field_copy(which, c):
        source, target = ((theta_hbm, theta), (speed_hbm, speed))[which]
        rows = pl.ds(c * CHUNK, CHUNK)
        return pltpu.make_async_copy(
            source.at[:, rows, :], target.at[:, rows, :], field_sems.at[which, c]
        )

    planes = [
        pltpu.make_async_copy(s, t, plane_sems.at[n])
        for n, (s, t) in enumerate(
            (
                (depth_hbm, depth),
                (zonal_hbm, zonal),
                (label_hbm, label),
                (energy_hbm, energy),
                (plan_hbm, plan),
            )
        )
    ]
    for copy in planes[:3]:
        copy.start()
    field_copy(0, 0).start()
    field_copy(1, 0).start()
    for copy in planes[3:]:
        copy.start()
    for c in range(1, chunks):
        field_copy(0, c).start()
        field_copy(1, c).start()

    row_id = lax.broadcasted_iota(jnp.int32, (ROWS, width), 0)
    last_row = row_id == ROWS - 1
    lane = lax.broadcasted_iota(jnp.int32, (ROWS, LANES), 1)

    def northern(own, beyond):
        return jnp.where(last_row, jnp.broadcast_to(beyond, own.shape), pltpu.roll(own, ROWS - 1, 0))

    class Block:
        def __init__(self, block, parts, basins):
            self.block, self.parts = block, parts
            self.rows = pl.ds(pl.multiple_of(block * ROWS, ROWS), ROWS)
            ahead = jnp.minimum(block + 1, blocks - 1) * ROWS
            self.beyond = pl.ds(pl.multiple_of(ahead, ROWS), ROWS)
            own_depth = depth[self.rows, :].astype(jnp.float32)
            next_depth = depth[self.beyond, :][0:1].astype(jnp.float32)
            next_depth = jnp.where(block == blocks - 1, 0.0, next_depth)
            self.face_depth = jnp.minimum(own_depth, northern(own_depth, next_depth))
            basin = label[self.rows, :]
            basins[...] = basin.astype(jnp.float32)
            self.in_basin = [basin == b for b in range(OCEAN_REGIONS)]
            self.span = zonal[self.rows, :]
            self.terms = jnp.zeros((ROWS, LANES), jnp.float32)
            self.running = [jnp.zeros((ROWS, 1), jnp.float32) for _ in range(OCEAN_REGIONS)]
            self.mean_sum = jnp.zeros((ROWS, width), jnp.float32)
            self.wet_sum = jnp.zeros((ROWS, width), jnp.float32)
            self.heat_sum = jnp.zeros((ROWS, width), jnp.float32)

        def level(self, k):
            own = theta[k, self.rows, :]
            face = 0.5 * (own + northern(own, theta[k, self.beyond, :][0:1]))
            volume = jnp.where(self.face_depth > float(k), tier[k] * self.span, 0.0)
            transport = volume * speed[k, self.rows, :]
            for q, value in enumerate(interpolation(face, transport)):
                self.parts[q, k] = value
            self.mean_sum += volume * face
            self.wet_sum += volume
            self.heat_sum += transport * face
            for b in range(OCEAN_REGIONS):
                self.running[b] += over_longitude(jnp.where(self.in_basin[b], transport, 0.0))
                self.terms = jnp.where(lane == b * levels + k, self.running[b], self.terms)

        def close(self):
            terms = self.terms
            total_flux = energy[self.rows, :] * plan[self.rows, :]
            for b in range(OCEAN_REGIONS):
                here = self.in_basin[b]
                heat = over_longitude(jnp.where(here, self.heat_sum, 0.0))
                terms = jnp.where(lane == HEAT + b, heat, terms)
                flux = over_longitude(jnp.where(here, total_flux, 0.0))
                terms = jnp.where(lane == FLUX + b, flux, terms)
            terms = jnp.where(lane == MEAN, over_longitude(self.mean_sum), terms)
            terms = jnp.where(lane == WET, over_longitude(self.wet_sum), terms)
            parcel[2 * self.block, TERMS : TERMS + 8, :] = terms
            parcel[2 * self.block + 1, TERMS : TERMS + 8, :] = pltpu.roll(terms, 4, 0)

    products = Products(width)

    def rows_of(parts, basins, block, fill):
        for pair in range(ROWS // 2):
            first = 2 * pair
            for k in range(first * levels // ROWS, (first + 2) * levels // ROWS):
                fill.level(k)
            spreads = [
                lambda q, k, count, r=r: jnp.broadcast_to(parts[q, k, r : r + 1, :], (count, width))
                for r in (first, first + 1)
            ]
            labels = [
                jnp.broadcast_to(basins[r : r + 1, :], (16, width)) for r in (first, first + 1)
            ]
            sums = products.pair(spreads, labels, levels)
            tile = class_tile(*sums)
            parcel[2 * block + pair // 2, 8 * (pair % 2) : 8 * (pair % 2) + 8, :] = tile
        fill.close()

    for copy in planes[:3]:
        copy.wait()
    field_copy(0, 0).wait()
    field_copy(1, 0).wait()
    opening = Block(jnp.int32(0), even, even_basins)
    for k in range(levels):
        opening.level(k)
    for copy in planes[3:]:
        copy.wait()
    opening.close()

    def two_blocks(i, carry):
        @pl.when(i < chunks - 1)
        def _():
            field_copy(0, i + 1).wait()
            field_copy(1, i + 1).wait()

        rows_of(even, even_basins, 2 * i, Block(2 * i + 1, odd, odd_basins))
        ahead = jnp.minimum(2 * i + 2, blocks - 1)
        rows_of(odd, odd_basins, 2 * i + 1, Block(ahead, even, even_basins))
        return carry

    lax.fori_loop(0, chunks, two_blocks, 0)

    final = parallels - 1
    half = width // 2
    span = zonal[final : final + 1, :]
    for k in range(levels):
        last[LAST_THETA + k : LAST_THETA + k + 1, :] = theta[k, final : final + 1, :]
        last[LAST_VOLUME + k : LAST_VOLUME + k + 1, :] = tier[k] * span
        last[LAST_SPEED + k : LAST_SPEED + k + 1, :] = speed[k, final : final + 1, :]
    for k in range(levels):
        south[k : k + 1, :] = theta[k, 0:1, :]
    south[levels : levels + 1, :] = depth[0:1, :].astype(jnp.float32)
    south[levels + 1 :, :] = jnp.zeros((EDGE - levels - 1, width), jnp.float32)
    last[LAST_DEPTH : LAST_DEPTH + 1, :] = depth[final : final + 1, :].astype(jnp.float32)
    last[LAST_BASIN : LAST_BASIN + 1, :] = label[final : final + 1, :].astype(jnp.float32)
    last[LAST_BASIN + 1 :, :] = jnp.zeros((LAST_ROWS - LAST_BASIN - 1, width), jnp.float32)
    totals = jnp.zeros((ROWS, LANES), jnp.float32)
    for d in range(0, 2 * blocks, 2):
        totals = totals + parcel[d, TERMS : TERMS + 8, :]
    totals = pltpu.roll(jnp.sum(totals, axis=0, keepdims=True), LANES // 4, 1)
    for d in range(2 * blocks):
        parcel[d, TOTALS : TOTALS + 1, :] = totals
        parcel[d, TOTALS + 1 : LEVEL, :] = jnp.zeros((LEVEL - TOTALS - 1, LANES), jnp.float32)
        for n, q in enumerate(
            (LAST_THETA + d, LAST_VOLUME + d, LAST_SPEED + d, LAST_DEPTH, LAST_BASIN)
        ):
            row = last[q : q + 1, :]
            parcel[d, LEVEL + 2 * n : LEVEL + 2 * n + 1, :] = row[:, :half]
            parcel[d, LEVEL + 2 * n + 1 : LEVEL + 2 * n + 2, :] = row[:, half:]


def last_kernel(lon_size, lat_size, seam, parcels, last, halo, share, parts):
    levels = EDGE - 8
    width = last.shape[1]
    devices = parcels.shape[0]
    lon_index = lax.axis_index("lon")
    at_fold = lax.axis_index("lat") == lat_size - 1
    start = seam[0] + lon_index * width + (lon_size * width - (width - 1))
    first, offset = start // width, start % width
    total = parcels[0, 0:LEVEL, :]
    for d in range(1, devices):
        total = total + parcels[d, 0:LEVEL, :]

    def whole_row(n):
        half = lambda h: jnp.concatenate(
            [parcels[d, LEVEL + 2 * n + h : LEVEL + 2 * n + h + 1, :] for d in range(devices)], axis=0
        )
        return jnp.concatenate([half(0), half(1)], axis=1)

    def mirrored(n):
        tiles = []
        for step in range(2):
            for h in range(2):
                at = LEVEL + 2 * n + h
                tiles.append(
                    jnp.concatenate(
                        [
                            parcels[(first + (step - d)) & (devices - 1), at : at + 1, :]
                            for d in range(devices)
                        ],
                        axis=0,
                    )
                )
        return jnp.concatenate(tiles, axis=1)

    high, rest = split_in_two(mirrored(0))
    middle, lowest = split_in_two(rest)
    source = lax.broadcasted_iota(jnp.int32, (2 * width, width), 0)
    target = lax.broadcasted_iota(jnp.int32, (2 * width, width), 1)
    mirror = jnp.where(source + target == offset + (width - 1), 1.0, 0.0).astype(jnp.bfloat16)
    pieces = jnp.dot(
        jnp.concatenate([high, middle, lowest, mirrored(3)], axis=0).astype(jnp.bfloat16),
        mirror,
        preferred_element_type=jnp.float32,
    )
    folded = pieces[0:16] + pieces[16:32] + pieces[32:48]

    spread_out = lambda row: jnp.broadcast_to(row, (levels, width))
    theta = jnp.where(at_fold, whole_row(0), last[LAST_THETA : LAST_THETA + levels, :])
    full_volume = jnp.where(at_fold, whole_row(1), last[LAST_VOLUME : LAST_VOLUME + levels, :])
    speed = jnp.where(at_fold, whole_row(2), last[LAST_SPEED : LAST_SPEED + levels, :])
    depth = jnp.where(at_fold, whole_row(3), spread_out(last[LAST_DEPTH : LAST_DEPTH + 1, :]))
    basin = jnp.where(at_fold, whole_row(4), spread_out(last[LAST_BASIN : LAST_BASIN + 1, :]))
    north = jnp.where(at_fold, folded, halo[0:levels, :])
    north_depth = jnp.where(at_fold, pieces[48:64], spread_out(halo[levels : levels + 1, :]))
    face = 0.5 * (theta + north)
    face_depth = jnp.minimum(depth, north_depth)
    row_id = lax.broadcasted_iota(jnp.int32, (levels, width), 0)
    level_id = jnp.where(at_fold, lon_index, row_id).astype(jnp.float32)
    volume = jnp.where(level_id < face_depth, full_volume, 0.0)
    transport = volume * speed
    for q, value in enumerate(interpolation(face, transport)):
        parts[q] = value
    parts[6] = basin
    products = Products(width)
    spread = lambda q, k, count: jnp.broadcast_to(parts[q, k : k + 1, :], (count, width))
    sums = products.alone(spread, lambda k: products.indicators(spread(6, k, 16)), levels)
    last_class = class_tile(sums, jnp.zeros_like(sums))

    lane = lax.broadcasted_iota(jnp.int32, (levels, LANES), 1)
    own_level = lax.broadcasted_iota(jnp.int32, (levels, LANES), 0)
    below = jnp.where(at_fold, lon_index, own_level) <= lane % levels
    heat = transport * face
    everything = lambda x: over_longitude(jnp.sum(x, axis=0, keepdims=True))
    running = jnp.zeros((levels, LANES), jnp.float32)
    lane1 = lane[0:1]
    terms = jnp.zeros((1, LANES), jnp.float32)
    for b in range(OCEAN_REGIONS):
        here = basin == float(b)
        level_sum = over_longitude(jnp.where(here, transport, 0.0))
        running = jnp.where((lane // levels == b) & below, level_sum, running)
        terms = jnp.where(lane1 == HEAT + b, everything(jnp.where(here, heat, 0.0)), terms)
    terms = jnp.where(lane1 == MEAN, everything(volume * face), terms)
    terms = jnp.where(lane1 == WET, everything(volume), terms)
    terms = terms + jnp.sum(running, axis=0, keepdims=True)

    place_id = lax.broadcasted_iota(jnp.int32, (EDGE, LANES), 0)
    lane24 = lax.broadcasted_iota(jnp.int32, (EDGE, LANES), 1)
    wanted = jnp.where(
        place_id < 16, (place_id & 1) * OCEAN_REGIONS + (place_id >> 2), place_id - 16
    )
    of_place = wanted == (lane24 >> 4)
    from_pair = jnp.where(place_id < 16, (place_id >> 1) & 1, 2)
    tiles = (total[0:8], total[8:16], last_class)
    wide = []
    for low in range(LOW):
        row = jnp.zeros((EDGE, LANES), jnp.float32)
        for n, tile in enumerate(tiles):
            row = jnp.where(
                of_place & (from_pair == n),
                jnp.broadcast_to(tile[low : low + 1], (EDGE, LANES)),
                row,
            )
        wide.append(row)
    wide_high, wide_low = split_in_two(jnp.concatenate(wide, axis=1))
    from_id = lax.broadcasted_iota(jnp.int32, (LANES, LANES), 0)
    to_id = lax.broadcasted_iota(jnp.int32, (LANES, LANES), 1)
    goal = (from_id & (HIGH - 1)) * LOW
    placing = jnp.concatenate(
        [jnp.where(to_id == goal + low, 1.0, 0.0) for low in range(LOW)], axis=0
    ).astype(jnp.bfloat16)
    placed = jnp.dot(
        jnp.concatenate([wide_high, wide_low], axis=0).astype(jnp.bfloat16),
        placing,
        preferred_element_type=jnp.float32,
    )
    placed = placed[0:EDGE] + placed[EDGE : 2 * EDGE]
    share[0:16, :] = placed[0:16]
    for n in range(4):
        own = pltpu.roll(terms, EXTRA - n * (LANES // 4), 1)
        share[TERMS + n : TERMS + n + 1, :] = jnp.where(
            lane1 >= EXTRA, own, total[TERMS + n : TERMS + n + 1]
        )
    share[LAST : LAST + 4, :] = placed[16:20]


def finish_kernel(unit_scale, implied_scale, shares, class_out, stream, heat, implied):
    devices = shares.shape[0]
    rows = 4 * devices
    levels = stream.shape[1]
    mine = shares[0, TERMS:SHARE, :]
    for d in range(1, devices):
        mine = mine + shares[d, TERMS:SHARE, :]
    lane = lax.broadcasted_iota(jnp.int32, (1, LANES), 1)
    own_terms = jnp.zeros((1, LANES), jnp.float32)
    for n in range(3):
        quarter = pltpu.roll(mine[n : n + 1], (n + 1) * (LANES // 4), 1)
        own_terms = jnp.where(lane // (LANES // 4) == n, quarter, own_terms)
    offsets = mine[3:4]
    for b in range(OCEAN_REGIONS):
        for d in range(devices):
            class_out[b, 4 * d : 4 * d + 4, :] = unit_scale * shares[d, 4 * b : 4 * b + 4, :]
        class_out[b, rows - 1 : rows, :] += unit_scale * mine[LAST - TERMS + b : LAST - TERMS + b + 1]
    terms = jnp.concatenate([shares[d, TERMS : TERMS + 4, :] for d in range(devices)], axis=0)
    row_id = lax.broadcasted_iota(jnp.int32, terms.shape, 0)
    terms = terms + jnp.where(row_id == rows - 1, jnp.broadcast_to(own_terms, terms.shape), 0.0)
    turned = jnp.transpose(
        jnp.concatenate([terms, jnp.zeros((LANES - rows, LANES), jnp.float32)], axis=0)
    )
    for b in range(OCEAN_REGIONS):
        stream[b] = unit_scale * turned[b * levels : (b + 1) * levels, :rows]
    row_mean = turned[MEAN : MEAN + 1] / jnp.where(lane < rows, turned[WET : WET + 1], 1.0)
    for b in range(OCEAN_REGIONS):
        total = turned[(b + 1) * levels - 1 : (b + 1) * levels]
        out = unit_scale / 16.0 * (turned[HEAT + b : HEAT + b + 1] - total * row_mean)
        heat[b : b + 1, :] = out[:, :rows]
        flux = turned[FLUX + b : FLUX + b + 1]
        offset = over_longitude(jnp.where(lane == FLUX + LANES // 4 + b, offsets, 0.0))
        shift = 1
        while shift < rows:
            flux = flux + jnp.where(lane >= shift, pltpu.roll(flux, shift, 1), 0.0)
            shift *= 2
        implied[b : b + 1, :] = (implied_scale * (flux + offset))[:, :rows]


def exchanged(pieces, axis):
    return lax.all_to_all(pieces, axis, split_axis=0, concat_axis=0, tiled=True)


def body(
    meridional_speed,
    theta_field,
    tier_vertical_span,
    grid_zonal_span,
    grid_plan_extent,
    ocean_energy_input,
    ocean_tier_tally,
    grid_region_label,
    seam_matching_meridian,
):
    levels, parallels, width = theta_field.shape
    lon_size = lax.axis_size("lon")
    lat_size = lax.axis_size("lat")
    width_total = width * lon_size
    unit_scale = math.sqrt(THERMAL_BINS / (width_total * levels))
    implied_scale = 2.0 / math.sqrt(width_total * parallels * lat_size)
    blocks = parallels // ROWS
    chunks = parallels // CHUNK

    in_smem = pl.BlockSpec(memory_space=pltpu.SMEM)
    in_vmem = pl.BlockSpec(memory_space=pltpu.VMEM)
    anywhere = pl.BlockSpec(memory_space=pl.ANY)
    plane_f32 = pltpu.VMEM((parallels, width), jnp.float32)
    plane_i32 = pltpu.VMEM((parallels, width), jnp.int32)
    field = pltpu.VMEM((levels, parallels, width), jnp.float32)
    parts = pltpu.VMEM((6, levels, ROWS, width), jnp.float32)
    parcels, last, southernmost = pl.pallas_call(
        rows_kernel,
        in_specs=[anywhere, anywhere, in_smem] + [anywhere] * 5,
        out_specs=(in_vmem,) * 3,
        out_shape=(
            jax.ShapeDtypeStruct((2 * blocks, PARCEL, LANES), jnp.float32),
            jax.ShapeDtypeStruct((LAST_ROWS, width), jnp.float32),
            jax.ShapeDtypeStruct((EDGE, width), jnp.float32),
        ),
        scratch_shapes=[
            field,
            field,
            plane_f32,
            plane_f32,
            plane_f32,
            plane_i32,
            plane_i32,
            parts,
            parts,
            pltpu.VMEM((ROWS, width), jnp.float32),
            pltpu.VMEM((ROWS, width), jnp.float32),
            pltpu.SemaphoreType.DMA((2, chunks)),
            pltpu.SemaphoreType.DMA((5,)),
        ],
        cost_estimate=pl.CostEstimate(
            flops=8_000_000_000, bytes_accessed=4_000_000, transcendentals=0
        ),
        name="rows",
    )(
        theta_field,
        meridional_speed,
        tier_vertical_span,
        grid_zonal_span,
        grid_plan_extent,
        ocean_energy_input,
        ocean_tier_tally,
        grid_region_label,
    )
    received = exchanged(parcels, "lon")
    halo = lax.ppermute(southernmost, "lat", [(i + 1, i) for i in range(lat_size - 1)])
    row_flux = jnp.sum(received[:, TOTALS, :], axis=0)[None]
    northward = [
        (r * lat_size + s, r * lat_size + s + r)
        for r in range(1, lon_size)
        for s in range(lat_size - r)
    ]
    of_block = lax.ppermute(row_flux, ("lon", "lat"), northward)
    share = pl.pallas_call(
        functools.partial(last_kernel, lon_size, lat_size),
        in_specs=[in_smem, in_vmem, in_vmem, in_vmem],
        out_specs=in_vmem,
        out_shape=jax.ShapeDtypeStruct((SHARE, LANES), jnp.float32),
        scratch_shapes=[
            pltpu.VMEM((7, levels, width), jnp.float32),
        ],
        compiler_params=pltpu.CompilerParams(vmem_limit_bytes=SMALL_KERNEL),
        cost_estimate=pl.CostEstimate(
            flops=1_000_000_000, bytes_accessed=600_000, transcendentals=0
        ),
        name="last_row",
    )(seam_matching_meridian, received, last, halo)
    row_id = lax.broadcasted_iota(jnp.int32, share.shape, 0)
    lane = lax.broadcasted_iota(jnp.int32, share.shape, 1)
    share = jnp.where((row_id == TERMS + 3) & (lane >= EXTRA), of_block, share)
    shares = exchanged(jnp.broadcast_to(share, (lon_size, SHARE, LANES)), "lon")
    class_out, stream, heat, implied = pl.pallas_call(
        functools.partial(finish_kernel, unit_scale, implied_scale),
        in_specs=[in_vmem],
        out_specs=(in_vmem,) * 4,
        out_shape=(
            jax.ShapeDtypeStruct((OCEAN_REGIONS, parallels, THERMAL_BINS), jnp.float32),
            jax.ShapeDtypeStruct((OCEAN_REGIONS, levels, parallels), jnp.float32),
            jax.ShapeDtypeStruct((OCEAN_REGIONS, parallels), jnp.float32),
            jax.ShapeDtypeStruct((OCEAN_REGIONS, parallels), jnp.float32),
        ),
        compiler_params=pltpu.CompilerParams(vmem_limit_bytes=SMALL_KERNEL),
        name="finish",
    )(shares)
    return class_out, jnp.transpose(stream, (0, 2, 1)), heat, implied


def solution(mesh):
    in_specs = (
        P(None, "lat", "lon"),
        P(None, "lat", "lon"),
        P(),
        P("lat", "lon"),
        P("lat", "lon"),
        P("lat", "lon"),
        P("lat", "lon"),
        P("lat", "lon"),
        P("lon"),
    )
    out_specs = (P(None, "lat", None), P(None, "lat", None), P(None, "lat"), P(None, "lat"))
    return jax.shard_map(body, mesh=mesh, in_specs=in_specs, out_specs=out_specs, check_vma=False)
```

```python
import functools
import math

import jax
import jax.numpy as jnp
from jax import lax
from jax.experimental import pallas as pl
from jax.experimental.pallas import tpu as pltpu
from jax.sharding import PartitionSpec as P

THERMAL_BINS = 128
OCEAN_REGIONS = 4
THERMAL_FLOOR = -2.0
THERMAL_RANGE = 32.0

ROWS = 8
CHUNK = 16
LOW = 8
HIGH = THERMAL_BINS // LOW
GROUPS = OCEAN_REGIONS * HIGH
LANES = 128
EDGE = 24
TERMS, TOTALS, LEVEL, PARCEL = 16, 20, 22, 32
LAST, SHARE = 20, 24
EXTRA = 96
SMALL_KERNEL = 8 * 1024 * 1024
LAST_THETA, LAST_VOLUME, LAST_SPEED, LAST_DEPTH, LAST_BASIN, LAST_ROWS = 0, 16, 32, 48, 49, 56
HEAT, FLUX, MEAN, WET = 64, 68, 76, 77


def split_in_two(x):
    high = x.astype(jnp.bfloat16).astype(jnp.float32)
    return high, x - high


def over_longitude(x):
    return jnp.sum(x, axis=1, keepdims=True)


def interpolation(face, transport):
    per_bin = THERMAL_BINS / THERMAL_RANGE
    position = jnp.clip((face - THERMAL_FLOOR) * per_bin, 0.0, THERMAL_BINS - 1.0)
    low_bin = jnp.minimum(jnp.floor(position), THERMAL_BINS - 2.0)
    digit = jnp.floor(low_bin * (1.0 / LOW))
    weighted = transport * (position - low_bin)
    return (
        digit,
        low_bin - LOW * digit,
        *split_in_two(transport),
        *split_in_two(weighted),
    )


class Products:
    def __init__(self, width):
        packed_id = lax.broadcasted_iota(jnp.int32, (16, width), 0)
        as_packed = lambda x: x.astype(jnp.float32).astype(jnp.bfloat16)
        self.high_ids = as_packed(packed_id)
        self.low_ids = as_packed(packed_id & (LOW - 1))
        self.one = jnp.ones((16, width), jnp.bfloat16)
        self.none = jnp.zeros((16, width), jnp.bfloat16)
        self.width = width

    def indicators(self, basin):
        basin = basin.astype(jnp.bfloat16)
        return [jnp.where(basin == b, self.one, self.none) for b in range(OCEAN_REGIONS)]

    def row(self, spread, in_basin, levels):
        values, groups = [], []
        for k in range(levels):
            at_high = spread(0, k, 16).astype(jnp.bfloat16) == self.high_ids
            at_high = jnp.where(at_high, self.one, self.none)
            groups.append(jnp.concatenate([at_high * x for x in in_basin(k)], axis=0))
            at_low = spread(1, k, 16).astype(jnp.bfloat16) == self.low_ids
            values.append(
                jnp.concatenate(
                    [
                        jnp.where(
                            at_low,
                            jnp.concatenate([spread(q, k, 8), spread(q + 1, k, 8)], axis=0).astype(
                                jnp.bfloat16
                            ),
                            self.none,
                        )
                        for q in (2, 4)
                    ],
                    axis=0,
                )
            )
        return values, groups

    def alone(self, spread, in_basin, levels):
        values, groups = self.row(spread, in_basin, levels)
        return lax.dot_general(
            jnp.concatenate(values, axis=1),
            jnp.concatenate(groups, axis=1),
            (((1,), (1,)), ((), ())),
            preferred_element_type=jnp.float32,
        )

    def pair(self, spreads, basins, levels):
        rows = []
        for spread, basin in zip(spreads, basins):
            here = self.indicators(basin)
            rows.append(self.row(spread, lambda k, here=here: here, levels))
        left = [g if n % 2 else v for n, (v, g) in enumerate(rows)]
        right = [v if n % 2 else g for n, (v, g) in enumerate(rows)]
        join = lambda sides: jnp.concatenate(
            [jnp.concatenate([side[k] for side in sides], axis=0) for k in range(levels)], axis=1
        )
        out = lax.dot_general(
            join(left), join(right), (((1,), (1,)), ((), ())), preferred_element_type=jnp.float32
        )
        sums = []
        for n in range(0, len(rows), 2):
            o = 96 * (n // 2)
            sums += [out[o : o + 32, o : o + 64], jnp.transpose(out[o + 32 : o + 96, o + 64 : o + 96])]
        return sums


def class_tile(first, second):
    both = jnp.concatenate([first, second], axis=1)
    plain = both[0:8] + both[8:16]
    upper = both[16:24] + both[24:32]
    moved = pltpu.roll(upper, 1, 0)
    low_id = lax.broadcasted_iota(jnp.int32, (LOW, LANES), 0)
    moved = jnp.where(low_id == 0, pltpu.roll(moved, 1, 1), moved)
    return plain - upper + moved


def rows_kernel(
    theta_hbm,
    speed_hbm,
    tier,
    zonal_hbm,
    plan_hbm,
    energy_hbm,
    depth_hbm,
    label_hbm,
    parcel,
    last,
    south,
    theta,
    speed,
    zonal,
    plan,
    energy,
    depth,
    label,
    even,
    odd,
    even_basins,
    odd_basins,
    field_sems,
    plane_sems,
):
    levels, parallels, width = theta.shape
    blocks = parallels // ROWS
    chunks = parallels // CHUNK

    def field_copy(which, c):
        source, target = ((theta_hbm, theta), (speed_hbm, speed))[which]
        rows = pl.ds(c * CHUNK, CHUNK)
        return pltpu.make_async_copy(
            source.at[:, rows, :], target.at[:, rows, :], field_sems.at[which, c]
        )

    planes = [
        pltpu.make_async_copy(s, t, plane_sems.at[n])
        for n, (s, t) in enumerate(
            (
                (depth_hbm, depth),
                (zonal_hbm, zonal),
                (label_hbm, label),
                (energy_hbm, energy),
                (plan_hbm, plan),
            )
        )
    ]
    for copy in planes[:3]:
        copy.start()
    field_copy(0, 0).start()
    field_copy(1, 0).start()
    for copy in planes[3:]:
        copy.start()
    for c in range(1, chunks):
        field_copy(0, c).start()
        field_copy(1, c).start()

    row_id = lax.broadcasted_iota(jnp.int32, (ROWS, width), 0)
    last_row = row_id == ROWS - 1
    lane = lax.broadcasted_iota(jnp.int32, (ROWS, LANES), 1)

    def northern(own, beyond):
        return jnp.where(last_row, jnp.broadcast_to(beyond, own.shape), pltpu.roll(own, ROWS - 1, 0))

    class Block:
        def __init__(self, block, parts, basins):
            self.block, self.parts = block, parts
            self.rows = pl.ds(block * ROWS, ROWS)
            ahead = min(block + 1, blocks - 1) * ROWS
            self.beyond = pl.ds(ahead, ROWS)
            own_depth = depth[self.rows, :].astype(jnp.float32)
            next_depth = depth[self.beyond, :][0:1].astype(jnp.float32)
            if block == blocks - 1:
                next_depth = jnp.zeros_like(next_depth)
            self.face_depth = jnp.minimum(own_depth, northern(own_depth, next_depth))
            basin = label[self.rows, :]
            basins[...] = basin.astype(jnp.float32)
            self.in_basin = [basin == b for b in range(OCEAN_REGIONS)]
            self.span = zonal[self.rows, :]
            self.terms = jnp.zeros((ROWS, LANES), jnp.float32)
            self.running = [jnp.zeros((ROWS, 1), jnp.float32) for _ in range(OCEAN_REGIONS)]
            self.mean_sum = jnp.zeros((ROWS, width), jnp.float32)
            self.wet_sum = jnp.zeros((ROWS, width), jnp.float32)
            self.heat_sum = jnp.zeros((ROWS, width), jnp.float32)

        def level(self, k):
            own = theta[k, self.rows, :]
            face = 0.5 * (own + northern(own, theta[k, self.beyond, :][0:1]))
            volume = jnp.where(self.face_depth > float(k), tier[k] * self.span, 0.0)
            transport = volume * speed[k, self.rows, :]
            for q, value in enumerate(interpolation(face, transport)):
                self.parts[q, k] = value
            self.mean_sum += volume * face
            self.wet_sum += volume
            self.heat_sum += transport * face
            for b in range(OCEAN_REGIONS):
                self.running[b] += over_longitude(jnp.where(self.in_basin[b], transport, 0.0))
                self.terms = jnp.where(lane == b * levels + k, self.running[b], self.terms)

        def close(self):
            terms = self.terms
            total_flux = energy[self.rows, :] * plan[self.rows, :]
            for b in range(OCEAN_REGIONS):
                here = self.in_basin[b]
                heat = over_longitude(jnp.where(here, self.heat_sum, 0.0))
                terms = jnp.where(lane == HEAT + b, heat, terms)
                flux = over_longitude(jnp.where(here, total_flux, 0.0))
                terms = jnp.where(lane == FLUX + b, flux, terms)
            terms = jnp.where(lane == MEAN, over_longitude(self.mean_sum), terms)
            terms = jnp.where(lane == WET, over_longitude(self.wet_sum), terms)
            parcel[2 * self.block, TERMS : TERMS + 8, :] = terms
            parcel[2 * self.block + 1, TERMS : TERMS + 8, :] = pltpu.roll(terms, 4, 0)

    products = Products(width)

    def rows_of(parts, basins, block, fill):
        for pair in range(ROWS // 2):
            first = 2 * pair
            if fill is not None:
                for k in range(first * levels // ROWS, (first + 2) * levels // ROWS):
                    fill.level(k)
            spreads = [
                lambda q, k, count, r=r: jnp.broadcast_to(parts[q, k, r : r + 1, :], (count, width))
                for r in (first, first + 1)
            ]
            labels = [
                jnp.broadcast_to(basins[r : r + 1, :], (16, width)) for r in (first, first + 1)
            ]
            sums = products.pair(spreads, labels, levels)
            tile = class_tile(*sums)
            parcel[2 * block + pair // 2, 8 * (pair % 2) : 8 * (pair % 2) + 8, :] = tile
        if fill is not None:
            fill.close()

    for copy in planes[:3]:
        copy.wait()
    field_copy(0, 0).wait()
    field_copy(1, 0).wait()
    opening = Block(0, even, even_basins)
    for k in range(levels):
        opening.level(k)
    for copy in planes[3:]:
        copy.wait()
    opening.close()

    for block in range(blocks):
        if block % 2 == 0 and block // 2 + 1 < chunks:
            field_copy(0, block // 2 + 1).wait()
            field_copy(1, block // 2 + 1).wait()
        now, ahead = ((even, even_basins), (odd, odd_basins))[:: 1 if block % 2 == 0 else -1]
        rows_of(*now, block, Block(block + 1, *ahead) if block + 1 < blocks else None)

    final = parallels - 1
    half = width // 2
    span = zonal[final : final + 1, :]
    for k in range(levels):
        last[LAST_THETA + k : LAST_THETA + k + 1, :] = theta[k, final : final + 1, :]
        last[LAST_VOLUME + k : LAST_VOLUME + k + 1, :] = tier[k] * span
        last[LAST_SPEED + k : LAST_SPEED + k + 1, :] = speed[k, final : final + 1, :]
    for k in range(levels):
        south[k : k + 1, :] = theta[k, 0:1, :]
    south[levels : levels + 1, :] = depth[0:1, :].astype(jnp.float32)
    south[levels + 1 :, :] = jnp.zeros((EDGE - levels - 1, width), jnp.float32)
    last[LAST_DEPTH : LAST_DEPTH + 1, :] = depth[final : final + 1, :].astype(jnp.float32)
    last[LAST_BASIN : LAST_BASIN + 1, :] = label[final : final + 1, :].astype(jnp.float32)
    last[LAST_BASIN + 1 :, :] = jnp.zeros((LAST_ROWS - LAST_BASIN - 1, width), jnp.float32)
    totals = jnp.zeros((ROWS, LANES), jnp.float32)
    for d in range(0, 2 * blocks, 2):
        totals = totals + parcel[d, TERMS : TERMS + 8, :]
    totals = pltpu.roll(jnp.sum(totals, axis=0, keepdims=True), LANES // 4, 1)
    for d in range(2 * blocks):
        parcel[d, TOTALS : TOTALS + 1, :] = totals
        parcel[d, TOTALS + 1 : LEVEL, :] = jnp.zeros((LEVEL - TOTALS - 1, LANES), jnp.float32)
        for n, q in enumerate(
            (LAST_THETA + d, LAST_VOLUME + d, LAST_SPEED + d, LAST_DEPTH, LAST_BASIN)
        ):
            row = last[q : q + 1, :]
            parcel[d, LEVEL + 2 * n : LEVEL + 2 * n + 1, :] = row[:, :half]
            parcel[d, LEVEL + 2 * n + 1 : LEVEL + 2 * n + 2, :] = row[:, half:]


def last_kernel(lon_size, lat_size, seam, parcels, last, halo, share, parts):
    levels = EDGE - 8
    width = last.shape[1]
    devices = parcels.shape[0]
    lon_index = lax.axis_index("lon")
    at_fold = lax.axis_index("lat") == lat_size - 1
    start = seam[0] + lon_index * width + (lon_size * width - (width - 1))
    first, offset = start // width, start % width
    total = parcels[0, 0:LEVEL, :]
    for d in range(1, devices):
        total = total + parcels[d, 0:LEVEL, :]

    def whole_row(n):
        half = lambda h: jnp.concatenate(
            [parcels[d, LEVEL + 2 * n + h : LEVEL + 2 * n + h + 1, :] for d in range(devices)], axis=0
        )
        return jnp.concatenate([half(0), half(1)], axis=1)

    def mirrored(n):
        tiles = []
        for step in range(2):
            for h in range(2):
                at = LEVEL + 2 * n + h
                tiles.append(
                    jnp.concatenate(
                        [
                            parcels[(first + (step - d)) & (devices - 1), at : at + 1, :]
                            for d in range(devices)
                        ],
                        axis=0,
                    )
                )
        return jnp.concatenate(tiles, axis=1)

    high, rest = split_in_two(mirrored(0))
    middle, lowest = split_in_two(rest)
    source = lax.broadcasted_iota(jnp.int32, (2 * width, width), 0)
    target = lax.broadcasted_iota(jnp.int32, (2 * width, width), 1)
    mirror = jnp.where(source + target == offset + (width - 1), 1.0, 0.0).astype(jnp.bfloat16)
    pieces = jnp.dot(
        jnp.concatenate([high, middle, lowest, mirrored(3)], axis=0).astype(jnp.bfloat16),
        mirror,
        preferred_element_type=jnp.float32,
    )
    folded = pieces[0:16] + pieces[16:32] + pieces[32:48]

    spread_out = lambda row: jnp.broadcast_to(row, (levels, width))
    theta = jnp.where(at_fold, whole_row(0), last[LAST_THETA : LAST_THETA + levels, :])
    full_volume = jnp.where(at_fold, whole_row(1), last[LAST_VOLUME : LAST_VOLUME + levels, :])
    speed = jnp.where(at_fold, whole_row(2), last[LAST_SPEED : LAST_SPEED + levels, :])
    depth = jnp.where(at_fold, whole_row(3), spread_out(last[LAST_DEPTH : LAST_DEPTH + 1, :]))
    basin = jnp.where(at_fold, whole_row(4), spread_out(last[LAST_BASIN : LAST_BASIN + 1, :]))
    north = jnp.where(at_fold, folded, halo[0:levels, :])
    north_depth = jnp.where(at_fold, pieces[48:64], spread_out(halo[levels : levels + 1, :]))
    face = 0.5 * (theta + north)
    face_depth = jnp.minimum(depth, north_depth)
    row_id = lax.broadcasted_iota(jnp.int32, (levels, width), 0)
    level_id = jnp.where(at_fold, lon_index, row_id).astype(jnp.float32)
    volume = jnp.where(level_id < face_depth, full_volume, 0.0)
    transport = volume * speed
    for q, value in enumerate(interpolation(face, transport)):
        parts[q] = value
    parts[6] = basin
    products = Products(width)
    spread = lambda q, k, count: jnp.broadcast_to(parts[q, k : k + 1, :], (count, width))
    sums = products.alone(spread, lambda k: products.indicators(spread(6, k, 16)), levels)
    last_class = class_tile(sums, jnp.zeros_like(sums))

    lane = lax.broadcasted_iota(jnp.int32, (levels, LANES), 1)
    own_level = lax.broadcasted_iota(jnp.int32, (levels, LANES), 0)
    below = jnp.where(at_fold, lon_index, own_level) <= lane % levels
    heat = transport * face
    everything = lambda x: over_longitude(jnp.sum(x, axis=0, keepdims=True))
    running = jnp.zeros((levels, LANES), jnp.float32)
    lane1 = lane[0:1]
    terms = jnp.zeros((1, LANES), jnp.float32)
    for b in range(OCEAN_REGIONS):
        here = basin == float(b)
        level_sum = over_longitude(jnp.where(here, transport, 0.0))
        running = jnp.where((lane // levels == b) & below, level_sum, running)
        terms = jnp.where(lane1 == HEAT + b, everything(jnp.where(here, heat, 0.0)), terms)
    terms = jnp.where(lane1 == MEAN, everything(volume * face), terms)
    terms = jnp.where(lane1 == WET, everything(volume), terms)
    terms = terms + jnp.sum(running, axis=0, keepdims=True)

    place_id = lax.broadcasted_iota(jnp.int32, (EDGE, LANES), 0)
    lane24 = lax.broadcasted_iota(jnp.int32, (EDGE, LANES), 1)
    wanted = jnp.where(
        place_id < 16, (place_id & 1) * OCEAN_REGIONS + (place_id >> 2), place_id - 16
    )
    of_place = wanted == (lane24 >> 4)
    from_pair = jnp.where(place_id < 16, (place_id >> 1) & 1, 2)
    tiles = (total[0:8], total[8:16], last_class)
    wide = []
    for low in range(LOW):
        row = jnp.zeros((EDGE, LANES), jnp.float32)
        for n, tile in enumerate(tiles):
            row = jnp.where(
                of_place & (from_pair == n),
                jnp.broadcast_to(tile[low : low + 1], (EDGE, LANES)),
                row,
            )
        wide.append(row)
    wide_high, wide_low = split_in_two(jnp.concatenate(wide, axis=1))
    from_id = lax.broadcasted_iota(jnp.int32, (LANES, LANES), 0)
    to_id = lax.broadcasted_iota(jnp.int32, (LANES, LANES), 1)
    goal = (from_id & (HIGH - 1)) * LOW
    placing = jnp.concatenate(
        [jnp.where(to_id == goal + low, 1.0, 0.0) for low in range(LOW)], axis=0
    ).astype(jnp.bfloat16)
    placed = jnp.dot(
        jnp.concatenate([wide_high, wide_low], axis=0).astype(jnp.bfloat16),
        placing,
        preferred_element_type=jnp.float32,
    )
    placed = placed[0:EDGE] + placed[EDGE : 2 * EDGE]
    share[0:16, :] = placed[0:16]
    for n in range(4):
        own = pltpu.roll(terms, EXTRA - n * (LANES // 4), 1)
        share[TERMS + n : TERMS + n + 1, :] = jnp.where(
            lane1 >= EXTRA, own, total[TERMS + n : TERMS + n + 1]
        )
    share[LAST : LAST + 4, :] = placed[16:20]


def finish_kernel(unit_scale, implied_scale, shares, class_out, stream, heat, implied):
    devices = shares.shape[0]
    rows = 4 * devices
    levels = stream.shape[1]
    mine = shares[0, TERMS:SHARE, :]
    for d in range(1, devices):
        mine = mine + shares[d, TERMS:SHARE, :]
    lane = lax.broadcasted_iota(jnp.int32, (1, LANES), 1)
    own_terms = jnp.zeros((1, LANES), jnp.float32)
    for n in range(3):
        quarter = pltpu.roll(mine[n : n + 1], (n + 1) * (LANES // 4), 1)
        own_terms = jnp.where(lane // (LANES // 4) == n, quarter, own_terms)
    offsets = mine[3:4]
    for b in range(OCEAN_REGIONS):
        for d in range(devices):
            class_out[b, 4 * d : 4 * d + 4, :] = unit_scale * shares[d, 4 * b : 4 * b + 4, :]
        class_out[b, rows - 1 : rows, :] += unit_scale * mine[LAST - TERMS + b : LAST - TERMS + b + 1]
    terms = jnp.concatenate([shares[d, TERMS : TERMS + 4, :] for d in range(devices)], axis=0)
    row_id = lax.broadcasted_iota(jnp.int32, terms.shape, 0)
    terms = terms + jnp.where(row_id == rows - 1, jnp.broadcast_to(own_terms, terms.shape), 0.0)
    turned = jnp.transpose(
        jnp.concatenate([terms, jnp.zeros((LANES - rows, LANES), jnp.float32)], axis=0)
    )
    for b in range(OCEAN_REGIONS):
        stream[b] = unit_scale * turned[b * levels : (b + 1) * levels, :rows]
    row_mean = turned[MEAN : MEAN + 1] / jnp.where(lane < rows, turned[WET : WET + 1], 1.0)
    for b in range(OCEAN_REGIONS):
        total = turned[(b + 1) * levels - 1 : (b + 1) * levels]
        out = unit_scale / 16.0 * (turned[HEAT + b : HEAT + b + 1] - total * row_mean)
        heat[b : b + 1, :] = out[:, :rows]
        flux = turned[FLUX + b : FLUX + b + 1]
        offset = over_longitude(jnp.where(lane == FLUX + LANES // 4 + b, offsets, 0.0))
        shift = 1
        while shift < rows:
            flux = flux + jnp.where(lane >= shift, pltpu.roll(flux, shift, 1), 0.0)
            shift *= 2
        implied[b : b + 1, :] = (implied_scale * (flux + offset))[:, :rows]


def exchanged(pieces, axis):
    return lax.all_to_all(pieces, axis, split_axis=0, concat_axis=0, tiled=True)


def body(
    meridional_speed,
    theta_field,
    tier_vertical_span,
    grid_zonal_span,
    grid_plan_extent,
    ocean_energy_input,
    ocean_tier_tally,
    grid_region_label,
    seam_matching_meridian,
):
    levels, parallels, width = theta_field.shape
    lon_size = lax.axis_size("lon")
    lat_size = lax.axis_size("lat")
    width_total = width * lon_size
    unit_scale = math.sqrt(THERMAL_BINS / (width_total * levels))
    implied_scale = 2.0 / math.sqrt(width_total * parallels * lat_size)
    blocks = parallels // ROWS
    chunks = parallels // CHUNK

    in_smem = pl.BlockSpec(memory_space=pltpu.SMEM)
    in_vmem = pl.BlockSpec(memory_space=pltpu.VMEM)
    anywhere = pl.BlockSpec(memory_space=pl.ANY)
    plane_f32 = pltpu.VMEM((parallels, width), jnp.float32)
    plane_i32 = pltpu.VMEM((parallels, width), jnp.int32)
    field = pltpu.VMEM((levels, parallels, width), jnp.float32)
    parts = pltpu.VMEM((6, levels, ROWS, width), jnp.float32)
    parcels, last, southernmost = pl.pallas_call(
        rows_kernel,
        in_specs=[anywhere, anywhere, in_smem] + [anywhere] * 5,
        out_specs=(in_vmem,) * 3,
        out_shape=(
            jax.ShapeDtypeStruct((2 * blocks, PARCEL, LANES), jnp.float32),
            jax.ShapeDtypeStruct((LAST_ROWS, width), jnp.float32),
            jax.ShapeDtypeStruct((EDGE, width), jnp.float32),
        ),
        scratch_shapes=[
            field,
            field,
            plane_f32,
            plane_f32,
            plane_f32,
            plane_i32,
            plane_i32,
            parts,
            parts,
            pltpu.VMEM((ROWS, width), jnp.float32),
            pltpu.VMEM((ROWS, width), jnp.float32),
            pltpu.SemaphoreType.DMA((2, chunks)),
            pltpu.SemaphoreType.DMA((5,)),
        ],
        cost_estimate=pl.CostEstimate(
            flops=8_000_000_000, bytes_accessed=4_000_000, transcendentals=0
        ),
        name="rows",
    )(
        theta_field,
        meridional_speed,
        tier_vertical_span,
        grid_zonal_span,
        grid_plan_extent,
        ocean_energy_input,
        ocean_tier_tally,
        grid_region_label,
    )
    received = exchanged(parcels, "lon")
    halo = lax.ppermute(southernmost, "lat", [(i + 1, i) for i in range(lat_size - 1)])
    row_flux = jnp.sum(received[:, TOTALS, :], axis=0)[None]
    northward = [
        (r * lat_size + s, r * lat_size + s + r)
        for r in range(1, lon_size)
        for s in range(lat_size - r)
    ]
    of_block = lax.ppermute(row_flux, ("lon", "lat"), northward)
    share = pl.pallas_call(
        functools.partial(last_kernel, lon_size, lat_size),
        in_specs=[in_smem, in_vmem, in_vmem, in_vmem],
        out_specs=in_vmem,
        out_shape=jax.ShapeDtypeStruct((SHARE, LANES), jnp.float32),
        scratch_shapes=[
            pltpu.VMEM((7, levels, width), jnp.float32),
        ],
        compiler_params=pltpu.CompilerParams(vmem_limit_bytes=SMALL_KERNEL),
        cost_estimate=pl.CostEstimate(
            flops=1_000_000_000, bytes_accessed=600_000, transcendentals=0
        ),
        name="last_row",
    )(seam_matching_meridian, received, last, halo)
    row_id = lax.broadcasted_iota(jnp.int32, share.shape, 0)
    lane = lax.broadcasted_iota(jnp.int32, share.shape, 1)
    share = jnp.where((row_id == TERMS + 3) & (lane >= EXTRA), of_block, share)
    shares = exchanged(jnp.broadcast_to(share, (lon_size, SHARE, LANES)), "lon")
    class_out, stream, heat, implied = pl.pallas_call(
        functools.partial(finish_kernel, unit_scale, implied_scale),
        in_specs=[in_vmem],
        out_specs=(in_vmem,) * 4,
        out_shape=(
            jax.ShapeDtypeStruct((OCEAN_REGIONS, parallels, THERMAL_BINS), jnp.float32),
            jax.ShapeDtypeStruct((OCEAN_REGIONS, levels, parallels), jnp.float32),
            jax.ShapeDtypeStruct((OCEAN_REGIONS, parallels), jnp.float32),
            jax.ShapeDtypeStruct((OCEAN_REGIONS, parallels), jnp.float32),
        ),
        compiler_params=pltpu.CompilerParams(vmem_limit_bytes=SMALL_KERNEL),
        name="finish",
    )(shares)
    return class_out, jnp.transpose(stream, (0, 2, 1)), heat, implied


def solution(mesh):
    in_specs = (
        P(None, "lat", "lon"),
        P(None, "lat", "lon"),
        P(),
        P("lat", "lon"),
        P("lat", "lon"),
        P("lat", "lon"),
        P("lat", "lon"),
        P("lat", "lon"),
        P("lon"),
    )
    out_specs = (P(None, "lat", None), P(None, "lat", None), P(None, "lat"), P(None, "lat"))
    return jax.shard_map(body, mesh=mesh, in_specs=in_specs, out_specs=out_specs, check_vma=False)
```
